256 devices in a mesh: node: 8 (over x, core), space: 32 (over y, z).
Axes of the slice: x: 4, y: 4, z: 8, core: 2. Of those that a mesh axis runs over, the one named last changes fastest.
Arguments:
- initial: float32 [128, 256, 256], P('space'), may hold values from -1 to 1
- kappa: float32 [128, 256, 256], P('space'), may hold values from 0.3 to 3
Outputs:
- sections: float32 [8, 128, 256, 256], P('node', 'space')
The draws below stay inside these ranges and needn't reach their ends.
All inputs are finite; a program needn't handle non-finite values.
Results may differ from the reference program's by a relative error of at most 0.0002.
Values sent between devices are 32-bit elements; how exact they have to be, the bound alone decides.
No kernel may reach another device: no remote copies, remote signals or barrier semaphores. Data moves between devices by JAX's collectives and lax.ppermute only.
A program may use at most 192 MiB of HBM per device.

```python
import math
import jax
import jax.numpy as jnp
from jax import lax

M = 8
NXY = 256
NZ = 128
SWEEPS = 2
VCYCLES = 2
SMOOTH = 2
LEVELS = 3
COARSE = 8


def level_of(own_key, shape, cuts, low, largest):
    gain = 1.0
    for axis_at, shards_of in cuts:
        heights = jax.random.uniform(jax.random.fold_in(jax.random.fold_in(own_key, 6), axis_at), (shards_of,), jnp.float32, low / len(cuts), largest / len(cuts))
        gain = gain * jnp.repeat(jnp.exp(heights), shape[axis_at] // shards_of).reshape((-1,) + (1,) * (len(shape) - 1 - axis_at))
    return gain


def setup_inputs(seed: int = 0) -> dict:
    splits = jax.random.split(jax.random.key(seed), 3)
    initial = jnp.clip(jax.random.uniform(splits[0], (NZ, NXY, NXY), jnp.float32, -1.0, 1.0) * level_of(splits[0], (NZ, NXY, NXY), ((0, 32),), -0.4, 0.0), -1.0, 1.0)
    kappa = jnp.clip(jnp.exp(math.log(3.0) - 2.3025851 * jax.random.uniform(splits[1], (NZ, NXY, NXY), jnp.float32) ** level_of(splits[1], (NZ, NXY, NXY), ((0, 32),), -0.2, 0.2)), 0.3, 3.0)
    return {"initial": initial, "kappa": kappa}


DIFFUSE = 2.0
REACT = 0.5
OMEGA = 0.8


def radau_gap(count, where):
    previous = 1.0
    current = where
    for degree in range(1, count):
        following = ((2 * degree + 1) * where * current - degree * previous) / (degree + 1)
        previous = current
        current = following
    return current - previous


def radau_table(count):
    zeros_found = []
    grid_count = 4096
    lower = -1.0
    value_low = radau_gap(count, lower)
    for place in range(1, grid_count):
        upper = -1.0 + 2.0 * place / grid_count
        value_up = radau_gap(count, upper)
        if value_low * value_up < 0.0:
            left_end = lower
            right_end = upper
            left_value = value_low
            for halving in range(100):
                middle = 0.5 * (left_end + right_end)
                middle_value = radau_gap(count, middle)
                if left_value * middle_value <= 0.0:
                    right_end = middle
                else:
                    left_end = middle
                    left_value = middle_value
            zeros_found.append(0.5 * (left_end + right_end))
        lower = upper
        value_low = value_up
    zeros_found.append(1.0)
    abscissa = [(value + 1.0) / 2.0 for value in zeros_found]
    table_rows = []
    for outer in range(count):
        table_rows.append([0.0] * count)
    for column in range(count):
        factor = [1.0]
        scale = 1.0
        for other in range(count):
            if other != column:
                widened = [0.0] * (len(factor) + 1)
                for power in range(len(factor)):
                    widened[power + 1] = widened[power + 1] + factor[power]
                    widened[power] = widened[power] - abscissa[other] * factor[power]
                factor = widened
                scale = scale * (abscissa[column] - abscissa[other])
        for outer in range(count):
            upto = abscissa[outer]
            accum = 0.0
            for power in range(len(factor)):
                accum = accum + factor[power] * upto ** (power + 1) / (power + 1)
            table_rows[outer][column] = accum / scale
    return abscissa, table_rows


def laplace(field):
    total = jnp.roll(field, -1, 1) + jnp.roll(field, 1, 1)
    total = total + jnp.roll(field, 1, 2) + jnp.roll(field, -1, 2)
    total = total + jnp.roll(field, 1, 3) + jnp.roll(field, -1, 3)
    return total - 6.0 * field


def smooth(field, source, shift):
    applied = field - shift * laplace(field)
    return field + OMEGA * (source - applied) / (1.0 + 6.0 * shift)


def restrict(field):
    a, b, c, d = field.shape
    return field.reshape(a, b // 2, 2, c // 2, 2, d // 2, 2).mean(axis=(2, 4, 6))


def prolong(field):
    return jnp.repeat(jnp.repeat(jnp.repeat(field, 2, 1), 2, 2), 2, 3)


def vcycle(level, field, source, shift):
    if level == LEVELS - 1:
        field = jnp.zeros_like(source)
        for sweep in range(COARSE):
            field = smooth(field, source, shift)
        return field
    if field is None:
        field = jnp.zeros_like(source)
    for sweep in range(SMOOTH):
        field = smooth(field, source, shift)
    remain = source - (field - shift * laplace(field))
    coarse_part = vcycle(level + 1, None, restrict(remain), shift / 4.0)
    field = field + prolong(coarse_part)
    for sweep in range(SMOOTH):
        field = smooth(field, source, shift)
    return field


def reference(initial, kappa):
    abscissa, table_rows = radau_table(M)
    quadrature = jnp.asarray(table_rows, jnp.float32)
    shift = jnp.asarray([DIFFUSE * value for value in abscissa], jnp.float32).reshape(M, 1, 1, 1)
    sections = jnp.broadcast_to(initial, (M,) + initial.shape).astype(jnp.float32)
    for sweep in range(SWEEPS):
        lap = laplace(sections)
        force = DIFFUSE * lap + REACT * kappa * (sections - sections * sections * sections)
        integral = jnp.einsum("mj,jzyx->mzyx", quadrature, force, precision=lax.Precision.HIGHEST)
        right = initial + integral - shift * lap
        for cycle in range(VCYCLES):
            sections = vcycle(0, sections, right, shift)
    return sections
```

```python
import functools

import jax
import jax.numpy as jnp
import ml_dtypes
import numpy as np
from jax import lax
from jax.experimental import pallas as pl
from jax.experimental.pallas import tpu as pltpu
from jax.sharding import PartitionSpec as P

DIFFUSE = 2.0
REACT = 0.5
OMEGA = 0.8
NODES = 8
SLABS = 32
PLANES = 4
NZ = 128
NXY = 256
VCYCLES = 2


def radau_gap(count, where):
    previous = 1.0
    current = where
    for degree in range(1, count):
        following = ((2 * degree + 1) * where * current - degree * previous) / (degree + 1)
        previous = current
        current = following
    return current - previous


def radau_table(count):
    zeros_found = []
    grid_count = 4096
    lower = -1.0
    value_low = radau_gap(count, lower)
    for place in range(1, grid_count):
        upper = -1.0 + 2.0 * place / grid_count
        value_up = radau_gap(count, upper)
        if value_low * value_up < 0.0:
            left_end = lower
            right_end = upper
            left_value = value_low
            for halving in range(100):
                middle = 0.5 * (left_end + right_end)
                middle_value = radau_gap(count, middle)
                if left_value * middle_value <= 0.0:
                    right_end = middle
                else:
                    left_end = middle
                    left_value = middle_value
            zeros_found.append(0.5 * (left_end + right_end))
        lower = upper
        value_low = value_up
    zeros_found.append(1.0)
    abscissa = [(value + 1.0) / 2.0 for value in zeros_found]
    table_rows = []
    for outer in range(count):
        table_rows.append([0.0] * count)
    for column in range(count):
        factor = [1.0]
        scale = 1.0
        for other in range(count):
            if other != column:
                widened = [0.0] * (len(factor) + 1)
                for power in range(len(factor)):
                    widened[power + 1] = widened[power + 1] + factor[power]
                    widened[power] = widened[power] - abscissa[other] * factor[power]
                factor = widened
                scale = scale * (abscissa[column] - abscissa[other])
        for outer in range(count):
            upto = abscissa[outer]
            accum = 0.0
            for power in range(len(factor)):
                accum = accum + factor[power] * upto ** (power + 1) / (power + 1)
            table_rows[outer][column] = accum / scale
    return (abscissa, table_rows)


def mode_list(n):
    return [("c", k) for k in range(n // 2)] + [("s", k) for k in range(1, n // 2 + 1)]


def mode_vector(n, kind, k):
    angle = 2.0 * np.pi * k * (np.arange(n) + 0.5) / n
    values = np.cos(angle) if kind == "c" else np.sin(angle)
    return values / np.sqrt((values * values).sum())


def child_mode(coarse, kind, k, which):
    if which == 0:
        return (kind, k)
    if kind == "c":
        return ("s", coarse) if k == 0 else ("c", coarse - k)
    return ("c", coarse // 2) if k == coarse // 2 else ("s", coarse - k)


def pair_mean(n):
    return np.kron(np.eye(n // 2), np.full((1, 2), 0.5))


def dimension_tables(n):
    mid, low = n // 2, n // 4
    basis = np.zeros((2, 2, low, n))
    basis1 = np.zeros((2, low, mid))
    basis2 = np.zeros((low, low))
    ring0, ring1, ring2 = np.zeros((2, 2, low)), np.zeros((2, low)), np.zeros(low)
    for i, (kind, k) in enumerate(mode_list(low)):
        basis2[i] = mode_vector(low, kind, k)
        ring2[i] = 2.0 * np.cos(2.0 * np.pi * k / low)
        for b in range(2):
            kind1, k1 = child_mode(low, kind, k, b)
            basis1[b, i] = mode_vector(mid, kind1, k1)
            ring1[b, i] = 2.0 * np.cos(2.0 * np.pi * k1 / mid)
            for a in range(2):
                kind0, k0 = child_mode(mid, kind1, k1, a)
                basis[a, b, i] = mode_vector(n, kind0, k0)
                ring0[a, b, i] = 2.0 * np.cos(2.0 * np.pi * k0 / n)
    mean0 = np.einsum("bin,abin->abi", basis1 @ pair_mean(n), basis)
    mean1 = np.einsum("in,bin->bi", basis2 @ pair_mean(mid), basis1)
    return basis, ring0, mean0, ring1, mean1, ring2


def halves(matrix):
    high = matrix.astype(ml_dtypes.bfloat16)
    rest = (matrix - high.astype(np.float64)).astype(ml_dtypes.bfloat16)
    return np.stack([high, rest])


@functools.lru_cache(maxsize=None)
def constants():
    basis, ring0, mean0, ring1, mean1, ring2 = dimension_tables(NXY)
    low = NXY // 4
    to_x = basis.reshape(2, 2, 4, 16, NXY).transpose(2, 0, 1, 3, 4).reshape(NXY, NXY)
    to_y = basis.transpose(1, 2, 0, 3).reshape(NXY, NXY)
    first_y = basis.transpose(1, 2, 0, 3).reshape(2, NODES, 16, NXY)
    first_y = first_y.transpose(1, 0, 2, 3).reshape(NODES, 32, NXY)

    zbasis, zring0, zmean0, zring1, zmean1, zring2 = dimension_tables(NZ)
    along = zbasis.reshape(NZ, SLABS, PLANES)
    to_z = np.einsum("ac,ksz->akszc", np.eye(2), along).reshape(2 * NZ, 2 * NZ)

    wide = lambda v: np.repeat(v[..., None], 128, axis=-1)
    zlev0 = np.stack([wide(zring0), wide(zmean0)])
    zlev1 = np.stack([wide(zring1), wide(zmean1)])
    zlev2 = wide(zring2)

    table = np.zeros((NODES * SLABS, 8, 128))
    for place in range(NODES * SLABS):
        kg, hq, inner, qb = place // 16, place // 8 % 2, place // 2 % 4, place % 2
        base = kg * 4 + inner
        q = hq * 2 + qb
        xs = slice(q * 16, q * 16 + 16)
        shape = (2, 2, 2, 16)
        over_x0 = lambda v: v[None, :, :, xs]
        over_x1 = lambda v: v[None, None, :, xs]
        for a in range(2):
            y0 = ring0[a, :, base].reshape(2, 1, 1, 1)
            table[place, a] = np.broadcast_to(y0 + over_x0(ring0), shape).reshape(128)
            r0 = mean0[a, :, base].reshape(2, 1, 1, 1)
            table[place, 2 + a] = np.broadcast_to(r0 * over_x0(mean0), shape).reshape(128)
        y1 = ring1[:, base].reshape(2, 1, 1, 1)
        table[place, 4] = np.broadcast_to(y1 + over_x1(ring1), shape).reshape(128)
        r1 = mean1[:, base].reshape(2, 1, 1, 1)
        table[place, 5] = np.broadcast_to(r1 * over_x1(mean1), shape).reshape(128)
        x2 = ring2[xs].reshape(1, 1, 1, 16)
        table[place, 6] = np.broadcast_to(ring2[base] + x2, shape).reshape(128)
    del low
    f32 = lambda v: np.asarray(v, np.float32)
    return {
        "x_fwd": halves(to_x.T.copy()),
        "x_inv": halves(to_x),
        "y_fwd": halves(to_y),
        "y_inv": halves(to_y.T.copy()),
        "y_first": halves(first_y),
        "z_fwd": halves(to_z),
        "z_inv": halves(to_z.T.copy()),
        "zlev0": f32(zlev0),
        "zlev1": f32(zlev1),
        "zlev2": f32(zlev2),
        "table": f32(table),
    }


def split(value):
    high = value.astype(jnp.bfloat16)
    return high, (value - high.astype(jnp.float32)).astype(jnp.bfloat16)


def product(a, b):
    return jnp.dot(a, b, preferred_element_type=jnp.float32)


def times(left, high, rest):
    a, b = split(left)
    return product(a, high) + product(b, high) + product(a, rest)


def apply(high, rest, right):
    a, b = split(right)
    return product(high, a) + product(high, b) + product(rest, a)


def exchange(low, high, shift, keep):
    size = low.shape[0 if shift < 8 else 1]
    axis = 0 if shift < 8 else 1
    first = jnp.where(keep, low, pltpu.roll(high, shift, axis))
    second = jnp.where(keep, pltpu.roll(low, size - shift, axis), high)
    return first, second


def shuffle_lanes(pairs):
    lane = lax.broadcasted_iota(jnp.int32, (8, 128), 1) < 64
    return [exchange(a, b, 64, lane) for a, b in pairs]


def shuffle_rows(four):
    row = lax.broadcasted_iota(jnp.int32, (8, 128), 0)
    top, even = row < 4, row % 4 < 2
    a0, b0 = exchange(four[0], four[2], 4, top)
    a1, b1 = exchange(four[1], four[3], 4, top)
    c0, c1 = exchange(a0, a1, 2, even)
    c2, c3 = exchange(b0, b1, 2, even)
    return [c0, c1, c2, c3]


def pack(read, write):
    pairs = shuffle_lanes([(read(z, 0), read(z, 1)) for z in range(PLANES)])
    for qb in range(2):
        for inner, chunk in enumerate(shuffle_rows([pairs[z][qb] for z in range(PLANES)])):
            write(inner, qb, chunk)


def unpack(read, write):
    columns = [shuffle_rows([read(inner, qb) for inner in range(4)]) for qb in range(2)]
    for z in range(PLANES):
        ((first, second),) = shuffle_lanes([(columns[0][z], columns[1][z])])
        write(z, 0, first)
        write(z, 1, second)


def cubic(u, strength):
    return REACT * strength * (u - u * u * u)


def first_kernel(node, u_ref, k_ref, x_fwd, y_first, out_ref, rows):
    me = node[0]
    for z in range(PLANES):
        u = u_ref[z]
        for array, field in enumerate((u, cubic(u, k_ref[z]))):
            part = times(field, x_fwd[0], x_fwd[1])
            part = apply(y_first[0, me], y_first[1, me], part)
            rows[array, z] = part.reshape(2, 16, NXY)
    for array in range(2):
        for g in range(2):
            for hq in range(2):
                lanes = slice(hq * 128, hq * 128 + 128)

                def read(z, b):
                    return rows[array, z, b, g * 8 : g * 8 + 8, lanes]

                def write(inner, qb, chunk):
                    out_ref[g, hq, inner, qb, array] = chunk

                pack(read, write)


def gather_rows(in_ref, rows):
    for kg in range(16):
        for hq in range(2):
            lanes = slice(hq * 128, hq * 128 + 128)

            def read(inner, qb):
                return in_ref[kg, hq, inner, qb]

            def write(z, b, tile):
                rows[z, b, kg * 8 : kg * 8 + 8, lanes] = tile

            unpack(read, write)


def scatter_rows(rows, out_ref):
    for kg in range(16):
        for hq in range(2):
            lanes = slice(hq * 128, hq * 128 + 128)

            def read(z, b):
                return rows[z, b, kg * 8 : kg * 8 + 8, lanes]

            def write(inner, qb, chunk):
                out_ref[kg, hq, inner, qb] = chunk

            pack(read, write)


def middle_kernel(in_ref, k_ref, x_fwd, x_inv, y_fwd, y_inv, out_ref, rows):
    gather_rows(in_ref, rows)
    for z in range(PLANES):
        part = apply(y_inv[0], y_inv[1], rows[z].reshape(NXY, NXY))
        u = times(part, x_inv[0], x_inv[1])
        part = times(cubic(u, k_ref[z]), x_fwd[0], x_fwd[1])
        rows[z] = apply(y_fwd[0], y_fwd[1], part).reshape(2, 128, NXY)
    scatter_rows(rows, out_ref)


def last_kernel(in_ref, x_inv, y_inv, out_ref, rows):
    gather_rows(in_ref, rows)
    for z in range(PLANES):
        part = apply(y_inv[0], y_inv[1], rows[z].reshape(NXY, NXY))
        out_ref[0, z] = times(part, x_inv[0], x_inv[1])


def lane_pair(value, distance, upper):
    if distance == 64:
        return value + pltpu.roll(value, 64, value.ndim - 1)
    ahead = pltpu.roll(value, 128 - distance, value.ndim - 1)
    behind = pltpu.roll(value, distance, value.ndim - 1)
    return value + jnp.where(upper, behind, ahead)


def mode_tables(group, zlev0, zlev1, zlev2, table):
    tile = pl.ds(group * 8, 8)
    row = lambda i: jnp.broadcast_to(table[0, i : i + 1, :], (8, 128))
    ring0 = [[[zlev0[0, c, d, tile] + row(a) for d in range(2)] for c in range(2)] for a in range(2)]
    mean0 = [[[zlev0[1, c, d, tile] * row(2 + a) for d in range(2)] for c in range(2)] for a in range(2)]
    ring1 = [zlev1[0, d, tile] + row(4) for d in range(2)]
    mean1 = [zlev1[1, d, tile] * row(5) for d in range(2)]
    ring2 = zlev2[tile] + row(6)
    three = lambda v: jnp.stack([jnp.stack([jnp.stack(y) for y in x]) for x in v])
    return three(ring0), three(mean0), jnp.stack(ring1), jnp.stack(mean1), ring2


def vcycles(tables, shifts, v, g):
    ring0, mean0, ring1, mean1, ring2 = tables
    lane = lax.broadcasted_iota(jnp.int32, (2, 8, 128), 2)
    upper32 = lane % 64 >= 32
    upper16 = (lane % 32 >= 16)[0]
    for cycle in range(VCYCLES):
        sums = []
        for m, s in enumerate(shifts):
            weight = OMEGA / (1.0 + 6.0 * s)
            sigma = (1.0 - OMEGA) + (weight * s) * ring0
            source = g[m]
            field = sigma * (sigma * v[m][...] + source[...]) + source[...]
            v[m][...] = field
            remain = mean0 * (source[...] + (sigma - 1.0) * field)
            sums.append((remain[0, 0] + remain[0, 1]) + (remain[1, 0] + remain[1, 1]))
        corrections = []
        for m, s in enumerate(shifts):
            weight = OMEGA / (1.0 + 6.0 * s)
            s1, s2 = s / 4.0, s / 16.0
            weight1, weight2 = OMEGA / (1.0 + 6.0 * s1), OMEGA / (1.0 + 6.0 * s2)
            sigma1 = (1.0 - OMEGA) + (weight1 * s1) * ring1
            sigma2 = (1.0 - OMEGA) + (weight2 * s2) * ring2
            source1 = (weight1 / weight) * lane_pair(sums[m], 32, upper32)
            square1 = sigma1 * sigma1
            remain1 = mean1 * square1 * source1
            total = lane_pair(remain1[0] + remain1[1], 64, None)
            source2 = (weight2 / weight1) * lane_pair(total, 16, upper16)
            square2 = sigma2 * sigma2
            coarse = (1.0 + sigma2) * (1.0 + square2) * (1.0 + square2 * square2) * source2
            smoothed = (1.0 + sigma1) * source1
            corrections.append(square1 * (smoothed + (8.0 * mean1) * coarse) + smoothed)
        for m, s in enumerate(shifts):
            weight = OMEGA / (1.0 + 6.0 * s)
            sigma = (1.0 - OMEGA) + (weight * s) * ring0
            source = g[m][...]
            field = v[m][...] + (8.0 * mean0) * corrections[m]
            v[m][...] = sigma * (sigma * field + source) + source


def to_slabs(modes, z_inv, out_ref):
    for pair in range(NODES // 2):
        both = jnp.concatenate(
            [modes[2 * pair + i].reshape(2 * NZ, 128) for i in range(2)], axis=1
        )
        both = apply(z_inv[0], z_inv[1], both)
        for i in range(2):
            out_ref[2 * pair + i] = both[:, i * 128 : i * 128 + 128].reshape(SLABS, 8, 128)


def start_kernel(
    shifts, sums, place, in_ref, z_fwd, z_inv, zlev0, zlev1, zlev2, table,
    out_ref, sections, start, cubes, v, g,
):
    both = jnp.concatenate([in_ref[:, i].reshape(2 * NZ, 128) for i in range(2)], axis=1)
    both = apply(z_fwd[0], z_fwd[1], both)
    start[...] = both[:, :128].reshape(2, 2, 2, 32, 128)
    cubes[...] = both[:, 128:].reshape(2, 2, 2, 32, 128)

    def group_step(group, carry):
        tables = mode_tables(group, zlev0, zlev1, zlev2, table)
        tile = pl.ds(group * 8, 8)
        lap = tables[0] - 6.0
        u = start[:, :, :, tile]
        force = DIFFUSE * lap * u + cubes[:, :, :, tile]
        for m, s in enumerate(shifts):
            right = u + sums[m] * force - s * (lap * u)
            g[m] = (OMEGA / (1.0 + 6.0 * s)) * right
            v[m] = u
        vcycles(tables, shifts, [v.at[m] for m in range(NODES)], [g.at[m] for m in range(NODES)])
        for m in range(NODES):
            sections[m, :, :, :, tile] = v[m]
        return carry

    lax.fori_loop(0, 4, group_step, 0)
    to_slabs(sections, z_inv, out_ref)


def step_kernel(
    shifts, quadrature, place, in_ref, sections, start, z_fwd, z_inv, zlev0, zlev1, zlev2, table,
    out_ref, cubes, force, v, g,
):
    for pair in range(NODES // 2):
        both = jnp.concatenate(
            [in_ref[2 * pair + i].reshape(2 * NZ, 128) for i in range(2)], axis=1
        )
        both = apply(z_fwd[0], z_fwd[1], both)
        for i in range(2):
            part = both[:, i * 128 : i * 128 + 128]
            cubes[2 * pair + i] = part.reshape(2, 2, 2, 32, 128)

    def group_step(group, carry):
        tables = mode_tables(group, zlev0, zlev1, zlev2, table)
        tile = pl.ds(group * 8, 8)
        lap = tables[0] - 6.0
        for m in range(NODES):
            force[m] = DIFFUSE * lap * sections[m, :, :, :, tile] + cubes[m, :, :, :, tile]
        for m, s in enumerate(shifts):
            u = sections[m, :, :, :, tile]
            right = start[:, :, :, tile] - s * (lap * u)
            for j in range(NODES):
                right = right + quadrature[m][j] * force[j]
            g[m] = (OMEGA / (1.0 + 6.0 * s)) * right
            v[m] = u
        vcycles(tables, shifts, [v.at[m] for m in range(NODES)], [g.at[m] for m in range(NODES)])
        for m in range(NODES):
            cubes[m, :, :, :, tile] = v[m]
        return carry

    lax.fori_loop(0, 4, group_step, 0)
    to_slabs(cubes, z_inv, out_ref)


def whole(shape):
    return pl.BlockSpec(shape, lambda *_: (0,) * len(shape))


def run(kernel, args, outs, scratch, scalar=None, table=None):
    specs = [whole(a.shape) for a in args]
    operands = list(args)
    if table is not None:
        specs.append(pl.BlockSpec((1, 8, 128), lambda i, place: (place[0], 0, 0)))
        operands.append(table)
    out_shape = [jax.ShapeDtypeStruct(shape, jnp.float32) for shape in outs]
    out_specs = [whole(shape) for shape in outs]
    grid_spec = pltpu.PrefetchScalarGridSpec(
        num_scalar_prefetch=0 if scalar is None else 1,
        grid=(1,),
        in_specs=specs,
        out_specs=out_specs,
        scratch_shapes=[pltpu.VMEM(shape, jnp.float32) for shape in scratch],
    )
    call = pl.pallas_call(
        kernel,
        grid_spec=grid_spec,
        out_shape=out_shape,
        compiler_params=pltpu.CompilerParams(vmem_limit_bytes=48 * 1024 * 1024),
    )
    return call(*([] if scalar is None else [scalar]), *operands)


def per_device(initial, kappa):
    abscissa, quadrature = radau_table(NODES)
    shifts = [DIFFUSE * value for value in abscissa]
    sums = [sum(row) for row in quadrature]
    c = {name: jnp.asarray(value) for name, value in constants().items()}
    node = lax.axis_index("node")
    place = (node * SLABS + lax.axis_index("space")).astype(jnp.int32).reshape(1)
    node = node.astype(jnp.int32).reshape(1)
    levels = (c["zlev0"], c["zlev1"], c["zlev2"])
    rows = (PLANES, 2, 128, NXY)
    tile = (2, 2, 2, 8, 128)
    modes = (2, 2, 2, 32, 128)

    (sent,) = run(
        first_kernel,
        (initial, kappa, c["x_fwd"], c["y_first"]),
        [(2, 2, 4, 2, 2, 8, 128)],
        [(2, PLANES, 2, 16, NXY)],
        scalar=node,
    )
    held = lax.all_to_all(sent.reshape(SLABS, 2, 8, 128), "space", 0, 0, tiled=True)
    sent, sections, start = run(
        functools.partial(start_kernel, shifts, sums),
        (held, c["z_fwd"], c["z_inv"], *levels),
        [(NODES, SLABS, 8, 128), (NODES,) + modes, modes],
        [modes, (NODES,) + tile, (NODES,) + tile],
        scalar=place,
        table=c["table"],
    )
    both = ("node", "space")
    count = NODES * SLABS
    held = lax.all_to_all(sent.reshape(count, 8, 128), both, 0, 0, tiled=True)
    (sent,) = run(
        middle_kernel,
        (held.reshape(16, 2, 4, 2, 8, 128), kappa, c["x_fwd"], c["x_inv"], c["y_fwd"], c["y_inv"]),
        [(16, 2, 4, 2, 8, 128)],
        [rows],
    )
    held = lax.all_to_all(sent.reshape(count, 8, 128), both, 0, 0, tiled=True)
    (sent,) = run(
        functools.partial(step_kernel, shifts, quadrature),
        (held.reshape(NODES, SLABS, 8, 128), sections, start, c["z_fwd"], c["z_inv"], *levels),
        [(NODES, SLABS, 8, 128)],
        [(NODES,) + modes, (NODES,) + tile, (NODES,) + tile, (NODES,) + tile],
        scalar=place,
        table=c["table"],
    )
    held = lax.all_to_all(sent.reshape(count, 8, 128), both, 0, 0, tiled=True)
    (out,) = run(
        last_kernel,
        (held.reshape(16, 2, 4, 2, 8, 128), c["x_inv"], c["y_inv"]),
        [(1, PLANES, NXY, NXY)],
        [rows],
    )
    return out


def solution(mesh):
    in_specs = (P("space", None, None), P("space", None, None))
    out_specs = P("node", "space", None, None)
    return jax.shard_map(
        per_device, mesh=mesh, in_specs=in_specs, out_specs=out_specs, check_vma=False
    )
```

```python
import functools

import jax
import jax.numpy as jnp
import ml_dtypes
import numpy as np
from jax import lax
from jax.experimental import pallas as pl
from jax.experimental.pallas import tpu as pltpu
from jax.sharding import PartitionSpec as P

DIFFUSE = 2.0
REACT = 0.5
OMEGA = 0.8
NODES = 8
SLABS = 32
PLANES = 4
NZ = 128
NXY = 256
VCYCLES = 2


def radau_gap(count, where):
    previous = 1.0
    current = where
    for degree in range(1, count):
        following = ((2 * degree + 1) * where * current - degree * previous) / (degree + 1)
        previous = current
        current = following
    return current - previous


def radau_table(count):
    zeros_found = []
    grid_count = 4096
    lower = -1.0
    value_low = radau_gap(count, lower)
    for place in range(1, grid_count):
        upper = -1.0 + 2.0 * place / grid_count
        value_up = radau_gap(count, upper)
        if value_low * value_up < 0.0:
            left_end = lower
            right_end = upper
            left_value = value_low
            for halving in range(100):
                middle = 0.5 * (left_end + right_end)
                middle_value = radau_gap(count, middle)
                if left_value * middle_value <= 0.0:
                    right_end = middle
                else:
                    left_end = middle
                    left_value = middle_value
            zeros_found.append(0.5 * (left_end + right_end))
        lower = upper
        value_low = value_up
    zeros_found.append(1.0)
    abscissa = [(value + 1.0) / 2.0 for value in zeros_found]
    table_rows = []
    for outer in range(count):
        table_rows.append([0.0] * count)
    for column in range(count):
        factor = [1.0]
        scale = 1.0
        for other in range(count):
            if other != column:
                widened = [0.0] * (len(factor) + 1)
                for power in range(len(factor)):
                    widened[power + 1] = widened[power + 1] + factor[power]
                    widened[power] = widened[power] - abscissa[other] * factor[power]
                factor = widened
                scale = scale * (abscissa[column] - abscissa[other])
        for outer in range(count):
            upto = abscissa[outer]
            accum = 0.0
            for power in range(len(factor)):
                accum = accum + factor[power] * upto ** (power + 1) / (power + 1)
            table_rows[outer][column] = accum / scale
    return (abscissa, table_rows)


def mode_list(n):
    return [("c", k) for k in range(n // 2)] + [("s", k) for k in range(1, n // 2 + 1)]


def mode_vector(n, kind, k):
    angle = 2.0 * np.pi * k * (np.arange(n) + 0.5) / n
    values = np.cos(angle) if kind == "c" else np.sin(angle)
    return values / np.sqrt((values * values).sum())


def child_mode(coarse, kind, k, which):
    if which == 0:
        return (kind, k)
    if kind == "c":
        return ("s", coarse) if k == 0 else ("c", coarse - k)
    return ("c", coarse // 2) if k == coarse // 2 else ("s", coarse - k)


def pair_mean(n):
    return np.kron(np.eye(n // 2), np.full((1, 2), 0.5))


def dimension_tables(n):
    mid, low = n // 2, n // 4
    basis = np.zeros((2, 2, low, n))
    basis1 = np.zeros((2, low, mid))
    basis2 = np.zeros((low, low))
    ring0, ring1, ring2 = np.zeros((2, 2, low)), np.zeros((2, low)), np.zeros(low)
    for i, (kind, k) in enumerate(mode_list(low)):
        basis2[i] = mode_vector(low, kind, k)
        ring2[i] = 2.0 * np.cos(2.0 * np.pi * k / low)
        for b in range(2):
            kind1, k1 = child_mode(low, kind, k, b)
            basis1[b, i] = mode_vector(mid, kind1, k1)
            ring1[b, i] = 2.0 * np.cos(2.0 * np.pi * k1 / mid)
            for a in range(2):
                kind0, k0 = child_mode(mid, kind1, k1, a)
                basis[a, b, i] = mode_vector(n, kind0, k0)
                ring0[a, b, i] = 2.0 * np.cos(2.0 * np.pi * k0 / n)
    mean0 = np.einsum("bin,abin->abi", basis1 @ pair_mean(n), basis)
    mean1 = np.einsum("in,bin->bi", basis2 @ pair_mean(mid), basis1)
    return basis, ring0, mean0, ring1, mean1, ring2


def halves(matrix):
    high = matrix.astype(ml_dtypes.bfloat16)
    rest = (matrix - high.astype(np.float64)).astype(ml_dtypes.bfloat16)
    return np.stack([high, rest])


@functools.lru_cache(maxsize=None)
def constants():
    basis, ring0, mean0, ring1, mean1, ring2 = dimension_tables(NXY)
    low = NXY // 4
    to_x = basis.reshape(2, 2, 4, 16, NXY).transpose(2, 0, 1, 3, 4).reshape(NXY, NXY)
    to_y = basis.transpose(1, 2, 0, 3).reshape(NXY, NXY)
    first_y = basis.transpose(1, 2, 0, 3).reshape(2, NODES, 16, NXY)
    first_y = first_y.transpose(1, 0, 2, 3).reshape(NODES, 32, NXY)

    zbasis, zring0, zmean0, zring1, zmean1, zring2 = dimension_tables(NZ)
    along = zbasis.reshape(NZ, SLABS, PLANES)
    to_z = np.einsum("ac,ksz->akszc", np.eye(2), along).reshape(2 * NZ, 2 * NZ)

    wide = lambda v: np.repeat(v[..., None], 128, axis=-1)
    zlev0 = np.stack([wide(zring0), wide(zmean0)])
    zlev1 = np.stack([wide(zring1), wide(zmean1)])
    zlev2 = wide(zring2)

    lanes = lambda v: np.broadcast_to(v, v.shape[:-4] + (2, 2, 2, 16)).reshape(v.shape[:-4] + (128,))
    ytable = np.zeros((low, 8, 128))
    for base in range(low):
        over_b = lambda v: lanes(v[:, base].reshape(2, 1, 1, 1))
        for a in range(2):
            ytable[base, a] = over_b(ring0[a])
            ytable[base, 2 + a] = over_b(mean0[a])
        ytable[base, 4] = over_b(ring1)
        ytable[base, 5] = over_b(mean1)
        ytable[base, 6] = ring2[base]
    xtable = np.zeros((4, 8, 128))
    for q in range(4):
        xs = slice(q * 16, q * 16 + 16)
        for a in range(2):
            xtable[q, a] = lanes(ring0[None, :, :, xs])
            xtable[q, 2 + a] = lanes(mean0[None, :, :, xs])
        xtable[q, 4] = lanes(ring1[None, None, :, xs])
        xtable[q, 5] = lanes(mean1[None, None, :, xs])
        xtable[q, 6] = lanes(ring2[None, None, None, xs])
    f32 = lambda v: np.asarray(v, np.float32)
    return {
        "x_fwd": halves(to_x.T.copy()),
        "x_inv": halves(to_x),
        "y_fwd": halves(to_y),
        "y_inv": halves(to_y.T.copy()),
        "y_first": np.concatenate([halves(first_y)[i] for i in (0, 0, 1)], axis=2),
        "z_fwd": halves(to_z),
        "z_inv": halves(to_z.T.copy()),
        "zlev0": f32(zlev0),
        "zlev1": f32(zlev1),
        "zlev2": f32(zlev2),
        "ytable": f32(ytable),
        "xtable": f32(xtable),
    }


def split(value):
    high = value.astype(jnp.bfloat16)
    return high, (value - high.astype(jnp.float32)).astype(jnp.bfloat16)


def product(a, b):
    return jnp.dot(a, b, preferred_element_type=jnp.float32)


def times(left, matrix):
    a, b = split(left)
    return product(
        jnp.concatenate([a, b, a], axis=1),
        jnp.concatenate([matrix[0], matrix[0], matrix[1]], axis=0),
    )


def apply(matrix, right):
    a, b = split(right)
    return product(
        jnp.concatenate([matrix[0], matrix[0], matrix[1]], axis=1),
        jnp.concatenate([a, b, a], axis=0),
    )


def exchange(low, high, shift, keep):
    size = low.shape[0 if shift < 8 else 1]
    axis = 0 if shift < 8 else 1
    first = jnp.where(keep, low, pltpu.roll(high, shift, axis))
    second = jnp.where(keep, pltpu.roll(low, size - shift, axis), high)
    return first, second


def shuffle_lanes(pairs):
    lane = lax.broadcasted_iota(jnp.int32, (8, 128), 1) < 64
    return [exchange(a, b, 64, lane) for a, b in pairs]


def shuffle_rows(four):
    row = lax.broadcasted_iota(jnp.int32, (8, 128), 0)
    top, even = row < 4, row % 4 < 2
    a0, b0 = exchange(four[0], four[2], 4, top)
    a1, b1 = exchange(four[1], four[3], 4, top)
    c0, c1 = exchange(a0, a1, 2, even)
    c2, c3 = exchange(b0, b1, 2, even)
    return [c0, c1, c2, c3]


def pack(read, write):
    pairs = shuffle_lanes([(read(z, 0), read(z, 1)) for z in range(PLANES)])
    for qb in range(2):
        for inner, chunk in enumerate(shuffle_rows([pairs[z][qb] for z in range(PLANES)])):
            write(inner, qb, chunk)


def unpack(read, write):
    columns = [shuffle_rows([read(inner, qb) for inner in range(4)]) for qb in range(2)]
    for z in range(PLANES):
        ((first, second),) = shuffle_lanes([(columns[0][z], columns[1][z])])
        write(z, 0, first)
        write(z, 1, second)


def cubic(u, strength):
    return REACT * strength * (u - u * u * u)


def first_kernel(
    node, u_far, k_far, x_far, y_far, out_ref, rows, part, u_near, k_near, x_near, y_near, sems
):
    me = node[0]
    copies = [pltpu.make_async_copy(y_far.at[me], y_near, sems.at[0])]
    for z in range(PLANES):
        copies.append(pltpu.make_async_copy(u_far.at[z], u_near.at[z], sems.at[2 * z + 1]))
        copies.append(pltpu.make_async_copy(k_far.at[z], k_near.at[z], sems.at[2 * z + 2]))
    copies.append(pltpu.make_async_copy(x_far, x_near, sems.at[9]))
    for copy in copies:
        copy.start()
    copies[0].wait()
    for z in range(PLANES):
        copies[2 * z + 1].wait()
        copies[2 * z + 2].wait()
        u = u_near[z]
        for array, field in enumerate((u, cubic(u, k_near[z]))):
            a, b = split(field)
            part[array, z] = product(y_near[...], jnp.concatenate([a, b, a], axis=0))
    copies[9].wait()
    for array in range(2):
        whole_part = times(part[array].reshape(PLANES * 32, NXY), x_near)
        rows[array] = whole_part.reshape(PLANES, 2, 16, NXY)
    for array in range(2):
        for g in range(2):
            for hq in range(2):
                lanes = slice(hq * 128, hq * 128 + 128)

                def read(z, b):
                    return rows[array, z, b, g * 8 : g * 8 + 8, lanes]

                def write(inner, qb, chunk):
                    out_ref[g, hq, inner, qb, array] = chunk

                pack(read, write)


def gather_rows(in_ref, rows):
    for kg in range(16):
        for hq in range(2):
            lanes = slice(hq * 128, hq * 128 + 128)

            def read(inner, qb):
                return in_ref[kg, hq, inner, qb]

            def write(z, b, tile):
                rows[z, b, kg * 8 : kg * 8 + 8, lanes] = tile

            unpack(read, write)


def scatter_rows(rows, out_ref):
    for kg in range(16):
        for hq in range(2):
            lanes = slice(hq * 128, hq * 128 + 128)

            def read(z, b):
                return rows[z, b, kg * 8 : kg * 8 + 8, lanes]

            def write(inner, qb, chunk):
                out_ref[kg, hq, inner, qb] = chunk

            pack(read, write)


def middle_kernel(in_ref, k_ref, x_fwd, x_inv, y_fwd, y_inv, out_ref, rows):
    gather_rows(in_ref, rows)
    for z in range(PLANES):
        part = apply(y_inv, rows[z].reshape(NXY, NXY))
        u = times(part, x_inv)
        part = times(cubic(u, k_ref[z]), x_fwd)
        rows[z] = apply(y_fwd, part).reshape(2, 128, NXY)
    scatter_rows(rows, out_ref)


def last_kernel(in_ref, x_inv, y_inv, out_ref, rows):
    gather_rows(in_ref, rows)
    for z in range(PLANES):
        part = apply(y_inv, rows[z].reshape(NXY, NXY))
        out_ref[0, z] = times(part, x_inv)


def lane_pair(value, distance, upper):
    if distance == 64:
        return value + pltpu.roll(value, 64, value.ndim - 1)
    ahead = pltpu.roll(value, 128 - distance, value.ndim - 1)
    behind = pltpu.roll(value, distance, value.ndim - 1)
    return value + jnp.where(upper, behind, ahead)


def mode_tables(group, zlev0, zlev1, zlev2, ytable, xtable):
    tile = pl.ds(group * 8, 8)

    def row(i, join):
        return jnp.broadcast_to(join(ytable[0, i : i + 1], xtable[0, i : i + 1]), (8, 128))

    total = [row(i, jnp.add) for i in (0, 1, 4, 6)]
    scale = [row(i, jnp.multiply) for i in (2, 3, 5)]
    ring0 = [[[zlev0[0, c, d, tile] + total[a] for d in range(2)] for c in range(2)] for a in range(2)]
    mean0 = [[[zlev0[1, c, d, tile] * scale[a] for d in range(2)] for c in range(2)] for a in range(2)]
    ring1 = [zlev1[0, d, tile] + total[2] for d in range(2)]
    mean1 = [zlev1[1, d, tile] * scale[2] for d in range(2)]
    ring2 = zlev2[tile] + total[3]
    three = lambda v: jnp.stack([jnp.stack([jnp.stack(y) for y in x]) for x in v])
    return three(ring0), three(mean0), jnp.stack(ring1), jnp.stack(mean1), ring2


def vcycles(tables, shifts, v, g, twice, drop):
    ring0, mean0, ring1, mean1, ring2 = tables
    lane = lax.broadcasted_iota(jnp.int32, (2, 8, 128), 2)
    upper32 = lane % 64 >= 32
    upper16 = (lane % 32 >= 16)[0]
    for m, s in enumerate(shifts):
        weight = OMEGA / (1.0 + 6.0 * s)
        sigma = (1.0 - OMEGA) + (weight * s) * ring0
        twice[m] = sigma * sigma
        drop[m] = mean0 * (sigma - 1.0)
        source = g[m]
        v[m] = sigma * (sigma * v[m] + source) + source
    for cycle in range(VCYCLES):
        sums = []
        for m in range(NODES):
            remain = mean0 * g[m] + drop[m] * v[m]
            sums.append((remain[0, 0] + remain[0, 1]) + (remain[1, 0] + remain[1, 1]))
        corrections = []
        for m, s in enumerate(shifts):
            weight = OMEGA / (1.0 + 6.0 * s)
            s1, s2 = s / 4.0, s / 16.0
            weight1, weight2 = OMEGA / (1.0 + 6.0 * s1), OMEGA / (1.0 + 6.0 * s2)
            sigma1 = (1.0 - OMEGA) + (weight1 * s1) * ring1
            sigma2 = (1.0 - OMEGA) + (weight2 * s2) * ring2
            source1 = (weight1 / weight) * lane_pair(sums[m], 32, upper32)
            square1 = sigma1 * sigma1
            remain1 = mean1 * square1 * source1
            total = lane_pair(remain1[0] + remain1[1], 64, None)
            source2 = (weight2 / weight1) * lane_pair(total, 16, upper16)
            square2 = sigma2 * sigma2
            coarse = (1.0 + sigma2) * (1.0 + square2) * (1.0 + square2 * square2) * source2
            smoothed = (1.0 + sigma1) * source1
            corrections.append(square1 * (8.0 * smoothed + (64.0 * mean1) * coarse) + 8.0 * smoothed)
        for m, s in enumerate(shifts):
            weight = OMEGA / (1.0 + 6.0 * s)
            sigma = (1.0 - OMEGA) + (weight * s) * ring0
            source = g[m] + sigma * g[m]
            field = twice[m] * (v[m] + mean0 * corrections[m]) + source
            if cycle + 1 < VCYCLES:
                field = twice[m] * field + source
            v[m] = field


def to_slabs(modes, z_inv, out_ref):
    for pair in range(NODES // 2):
        both = jnp.concatenate(
            [modes[2 * pair + i].reshape(2 * NZ, 128) for i in range(2)], axis=1
        )
        both = apply(z_inv, both)
        for i in range(2):
            out_ref[2 * pair + i] = both[:, i * 128 : i * 128 + 128].reshape(SLABS, 8, 128)


def start_kernel(
    shifts, sums, place, in_ref, z_fwd, z_inv, zlev0, zlev1, zlev2, ytable, xtable,
    out_ref, sections, start, cubes, v, g, twice, drop,
):
    both = jnp.concatenate([in_ref[:, i].reshape(2 * NZ, 128) for i in range(2)], axis=1)
    both = apply(z_fwd, both)
    start[...] = both[:, :128].reshape(2, 2, 2, 32, 128)
    cubes[...] = both[:, 128:].reshape(2, 2, 2, 32, 128)

    def group_step(group, carry):
        tables = mode_tables(group, zlev0, zlev1, zlev2, ytable, xtable)
        tile = pl.ds(group * 8, 8)
        lap = tables[0] - 6.0
        u = start[:, :, :, tile]
        force = DIFFUSE * lap * u + cubes[:, :, :, tile]
        for m, s in enumerate(shifts):
            right = u + sums[m] * force - s * (lap * u)
            g[m] = (OMEGA / (1.0 + 6.0 * s)) * right
            v[m] = u
        vcycles(tables, shifts, v, g, twice, drop)
        for m in range(NODES):
            sections[m, :, :, :, tile] = v[m]
        return carry

    lax.fori_loop(0, 4, group_step, 0)
    to_slabs(sections, z_inv, out_ref)


def step_kernel(
    shifts, quadrature, place, in_ref, sections, start, z_fwd, z_inv, zlev0, zlev1, zlev2, ytable, xtable,
    out_ref, cubes, force, v, g, twice, drop,
):
    for pair in range(NODES // 2):
        both = jnp.concatenate(
            [in_ref[2 * pair + i].reshape(2 * NZ, 128) for i in range(2)], axis=1
        )
        both = apply(z_fwd, both)
        for i in range(2):
            part = both[:, i * 128 : i * 128 + 128]
            cubes[2 * pair + i] = part.reshape(2, 2, 2, 32, 128)

    def group_step(group, carry):
        tables = mode_tables(group, zlev0, zlev1, zlev2, ytable, xtable)
        tile = pl.ds(group * 8, 8)
        lap = tables[0] - 6.0
        for m in range(NODES):
            force[m] = DIFFUSE * lap * sections[m, :, :, :, tile] + cubes[m, :, :, :, tile]
        for m, s in enumerate(shifts):
            u = sections[m, :, :, :, tile]
            right = start[:, :, :, tile] - s * (lap * u)
            for j in range(NODES):
                right = right + quadrature[m][j] * force[j]
            g[m] = (OMEGA / (1.0 + 6.0 * s)) * right
            v[m] = u
        vcycles(tables, shifts, v, g, twice, drop)
        for m in range(NODES):
            cubes[m, :, :, :, tile] = v[m]
        return carry

    lax.fori_loop(0, 4, group_step, 0)
    to_slabs(cubes, z_inv, out_ref)


def whole(shape):
    return pl.BlockSpec(shape, lambda *_: (0,) * len(shape))


FAR = pl.BlockSpec(memory_space=pltpu.MemorySpace.HBM)


def run(kernel, args, outs, scratch, scalar=None, tables=(), far=False):
    specs = [FAR if far else whole(a.shape) for a in args]
    if tables:
        base = lambda i, place: (place[0] // 16 * 4 + place[0] // 2 % 4, 0, 0)
        part = lambda i, place: (place[0] // 8 % 2 * 2 + place[0] % 2, 0, 0)
        specs += [pl.BlockSpec((1, 8, 128), base), pl.BlockSpec((1, 8, 128), part)]
    out_shape = [jax.ShapeDtypeStruct(shape, jnp.float32) for shape in outs]
    out_specs = [whole(shape) for shape in outs]
    grid_spec = pltpu.PrefetchScalarGridSpec(
        num_scalar_prefetch=0 if scalar is None else 1,
        grid=(1,),
        in_specs=specs,
        out_specs=out_specs,
        scratch_shapes=[pltpu.VMEM(s, jnp.float32) if isinstance(s, tuple) else s for s in scratch],
    )
    call = pl.pallas_call(
        kernel,
        grid_spec=grid_spec,
        out_shape=out_shape,
        compiler_params=pltpu.CompilerParams(vmem_limit_bytes=48 * 1024 * 1024),
    )
    if far:
        args = [pltpu.with_memory_space_constraint(a, pltpu.MemorySpace.HBM) for a in args]
    return call(*([] if scalar is None else [scalar]), *args, *tables)


def per_device(initial, kappa):
    abscissa, quadrature = radau_table(NODES)
    shifts = [DIFFUSE * value for value in abscissa]
    sums = [sum(row) for row in quadrature]
    c = {name: jnp.asarray(value) for name, value in constants().items()}
    node = lax.axis_index("node")
    place = (node * SLABS + lax.axis_index("space")).astype(jnp.int32).reshape(1)
    node = node.astype(jnp.int32).reshape(1)
    levels = (c["zlev0"], c["zlev1"], c["zlev2"])
    rows = (PLANES, 2, 128, NXY)
    tile = (2, 2, 2, 8, 128)
    modes = (2, 2, 2, 32, 128)

    (sent,) = run(
        first_kernel,
        (initial, kappa, c["x_fwd"], c["y_first"]),
        [(2, 2, 4, 2, 2, 8, 128)],
        [
            (2, PLANES, 2, 16, NXY),
            (2, PLANES, 32, NXY),
            (PLANES, NXY, NXY),
            (PLANES, NXY, NXY),
            pltpu.VMEM((2, NXY, NXY), jnp.bfloat16),
            pltpu.VMEM((32, 3 * NXY), jnp.bfloat16),
            pltpu.SemaphoreType.DMA((10,)),
        ],
        scalar=node,
        far=True,
    )
    held = lax.all_to_all(sent.reshape(SLABS, 2, 8, 128), "space", 0, 0, tiled=True)
    sent, sections, start = run(
        functools.partial(start_kernel, shifts, sums),
        (held, c["z_fwd"], c["z_inv"], *levels),
        [(NODES, SLABS, 8, 128), (NODES,) + modes, modes],
        [modes] + [(NODES,) + tile] * 4,
        scalar=place,
        tables=(c["ytable"], c["xtable"]),
    )
    both = ("node", "space")
    count = NODES * SLABS
    held = lax.all_to_all(sent.reshape(count, 8, 128), both, 0, 0, tiled=True)
    (sent,) = run(
        middle_kernel,
        (held.reshape(16, 2, 4, 2, 8, 128), kappa, c["x_fwd"], c["x_inv"], c["y_fwd"], c["y_inv"]),
        [(16, 2, 4, 2, 8, 128)],
        [rows],
    )
    held = lax.all_to_all(sent.reshape(count, 8, 128), both, 0, 0, tiled=True)
    (sent,) = run(
        functools.partial(step_kernel, shifts, quadrature),
        (held.reshape(NODES, SLABS, 8, 128), sections, start, c["z_fwd"], c["z_inv"], *levels),
        [(NODES, SLABS, 8, 128)],
        [(NODES,) + modes] + [(NODES,) + tile] * 5,
        scalar=place,
        tables=(c["ytable"], c["xtable"]),
    )
    held = lax.all_to_all(sent.reshape(count, 8, 128), both, 0, 0, tiled=True)
    (out,) = run(
        last_kernel,
        (held.reshape(16, 2, 4, 2, 8, 128), c["x_inv"], c["y_inv"]),
        [(1, PLANES, NXY, NXY)],
        [rows],
    )
    return out


def solution(mesh):
    in_specs = (P("space", None, None), P("space", None, None))
    out_specs = P("node", "space", None, None)
    return jax.shard_map(
        per_device, mesh=mesh, in_specs=in_specs, out_specs=out_specs, check_vma=False
    )
```

```python
import functools

import jax
import jax.numpy as jnp
import ml_dtypes
import numpy as np
from jax import lax
from jax.experimental import pallas as pl
from jax.experimental.pallas import tpu as pltpu
from jax.sharding import PartitionSpec as P

DIFFUSE = 2.0
REACT = 0.5
OMEGA = 0.8
NODES = 8
SLABS = 32
PLANES = 4
NZ = 128
NXY = 256
VCYCLES = 2


def radau_gap(count, where):
    previous = 1.0
    current = where
    for degree in range(1, count):
        following = ((2 * degree + 1) * where * current - degree * previous) / (degree + 1)
        previous = current
        current = following
    return current - previous


def radau_table(count):
    zeros_found = []
    grid_count = 4096
    lower = -1.0
    value_low = radau_gap(count, lower)
    for place in range(1, grid_count):
        upper = -1.0 + 2.0 * place / grid_count
        value_up = radau_gap(count, upper)
        if value_low * value_up < 0.0:
            left_end = lower
            right_end = upper
            left_value = value_low
            for halving in range(100):
                middle = 0.5 * (left_end + right_end)
                middle_value = radau_gap(count, middle)
                if left_value * middle_value <= 0.0:
                    right_end = middle
                else:
                    left_end = middle
                    left_value = middle_value
            zeros_found.append(0.5 * (left_end + right_end))
        lower = upper
        value_low = value_up
    zeros_found.append(1.0)
    abscissa = [(value + 1.0) / 2.0 for value in zeros_found]
    table_rows = []
    for outer in range(count):
        table_rows.append([0.0] * count)
    for column in range(count):
        factor = [1.0]
        scale = 1.0
        for other in range(count):
            if other != column:
                widened = [0.0] * (len(factor) + 1)
                for power in range(len(factor)):
                    widened[power + 1] = widened[power + 1] + factor[power]
                    widened[power] = widened[power] - abscissa[other] * factor[power]
                factor = widened
                scale = scale * (abscissa[column] - abscissa[other])
        for outer in range(count):
            upto = abscissa[outer]
            accum = 0.0
            for power in range(len(factor)):
                accum = accum + factor[power] * upto ** (power + 1) / (power + 1)
            table_rows[outer][column] = accum / scale
    return (abscissa, table_rows)


def mode_list(n):
    return [("c", k) for k in range(n // 2)] + [("s", k) for k in range(1, n // 2 + 1)]


def mode_vector(n, kind, k):
    angle = 2.0 * np.pi * k * (np.arange(n) + 0.5) / n
    values = np.cos(angle) if kind == "c" else np.sin(angle)
    return values / np.sqrt((values * values).sum())


def child_mode(coarse, kind, k, which):
    if which == 0:
        return (kind, k)
    if kind == "c":
        return ("s", coarse) if k == 0 else ("c", coarse - k)
    return ("c", coarse // 2) if k == coarse // 2 else ("s", coarse - k)


def pair_mean(n):
    return np.kron(np.eye(n // 2), np.full((1, 2), 0.5))


def dimension_tables(n):
    mid, low = n // 2, n // 4
    basis = np.zeros((2, 2, low, n))
    basis1 = np.zeros((2, low, mid))
    basis2 = np.zeros((low, low))
    ring0, ring1, ring2 = np.zeros((2, 2, low)), np.zeros((2, low)), np.zeros(low)
    for i, (kind, k) in enumerate(mode_list(low)):
        basis2[i] = mode_vector(low, kind, k)
        ring2[i] = 2.0 * np.cos(2.0 * np.pi * k / low)
        for b in range(2):
            kind1, k1 = child_mode(low, kind, k, b)
            basis1[b, i] = mode_vector(mid, kind1, k1)
            ring1[b, i] = 2.0 * np.cos(2.0 * np.pi * k1 / mid)
            for a in range(2):
                kind0, k0 = child_mode(mid, kind1, k1, a)
                basis[a, b, i] = mode_vector(n, kind0, k0)
                ring0[a, b, i] = 2.0 * np.cos(2.0 * np.pi * k0 / n)
    mean0 = np.einsum("bin,abin->abi", basis1 @ pair_mean(n), basis)
    mean1 = np.einsum("in,bin->bi", basis2 @ pair_mean(mid), basis1)
    return basis, ring0, mean0, ring1, mean1, ring2


def halves(matrix):
    high = matrix.astype(ml_dtypes.bfloat16)
    rest = (matrix - high.astype(np.float64)).astype(ml_dtypes.bfloat16)
    return np.stack([high, rest])


@functools.lru_cache(maxsize=None)
def constants():
    basis, ring0, mean0, ring1, mean1, ring2 = dimension_tables(NXY)
    low = NXY // 4
    to_x = basis.reshape(2, 2, 4, 16, NXY).transpose(2, 0, 1, 3, 4).reshape(NXY, NXY)
    to_y = basis.transpose(1, 2, 0, 3).reshape(NXY, NXY)
    first_y = basis.transpose(1, 2, 0, 3).reshape(2, NODES, 16, NXY)
    first_y = first_y.transpose(1, 0, 2, 3).reshape(NODES, 32, NXY)

    zbasis, zring0, zmean0, zring1, zmean1, zring2 = dimension_tables(NZ)
    along = zbasis.reshape(NZ, SLABS, PLANES)
    to_z = np.einsum("ac,ksz->akszc", np.eye(2), along).reshape(2 * NZ, 2 * NZ)

    wide = lambda v: np.repeat(v[..., None], 128, axis=-1)
    zlev0 = np.stack([wide(zring0), wide(zmean0)])
    zlev1 = np.stack([wide(zring1), wide(zmean1)])
    zlev2 = wide(zring2)

    lanes = lambda v: np.broadcast_to(v, v.shape[:-4] + (2, 2, 2, 16)).reshape(v.shape[:-4] + (128,))
    ytable = np.zeros((low, 8, 128))
    for base in range(low):
        over_b = lambda v: lanes(v[:, base].reshape(2, 1, 1, 1))
        for a in range(2):
            ytable[base, a] = over_b(ring0[a])
            ytable[base, 2 + a] = over_b(mean0[a])
        ytable[base, 4] = over_b(ring1)
        ytable[base, 5] = over_b(mean1)
        ytable[base, 6] = ring2[base]
    xtable = np.zeros((4, 8, 128))
    for q in range(4):
        xs = slice(q * 16, q * 16 + 16)
        for a in range(2):
            xtable[q, a] = lanes(ring0[None, :, :, xs])
            xtable[q, 2 + a] = lanes(mean0[None, :, :, xs])
        xtable[q, 4] = lanes(ring1[None, None, :, xs])
        xtable[q, 5] = lanes(mean1[None, None, :, xs])
        xtable[q, 6] = lanes(ring2[None, None, None, xs])
    f32 = lambda v: np.asarray(v, np.float32)
    return {
        "x_fwd": halves(to_x.T.copy()),
        "x_inv": halves(to_x),
        "y_fwd": halves(to_y),
        "y_inv": halves(to_y.T.copy()),
        "y_first": np.concatenate([halves(first_y)[i] for i in (0, 0, 1)], axis=2),
        "z_fwd": halves(to_z),
        "z_inv": halves(to_z.T.copy()),
        "zlev0": f32(zlev0),
        "zlev1": f32(zlev1),
        "zlev2": f32(zlev2),
        "ytable": f32(ytable),
        "xtable": f32(xtable),
    }


def split(value):
    high = value.astype(jnp.bfloat16)
    return high, (value - high.astype(jnp.float32)).astype(jnp.bfloat16)


def product(a, b):
    return jnp.dot(a, b, preferred_element_type=jnp.float32)


def times(left, matrix):
    a, b = split(left)
    return product(
        jnp.concatenate([a, b, a], axis=1),
        jnp.concatenate([matrix[0], matrix[0], matrix[1]], axis=0),
    )


def apply(matrix, right):
    a, b = split(right)
    return product(
        jnp.concatenate([matrix[0], matrix[0], matrix[1]], axis=1),
        jnp.concatenate([a, b, a], axis=0),
    )


def exchange(low, high, shift, keep):
    size = low.shape[0 if shift < 8 else 1]
    axis = 0 if shift < 8 else 1
    first = jnp.where(keep, low, pltpu.roll(high, shift, axis))
    second = jnp.where(keep, pltpu.roll(low, size - shift, axis), high)
    return first, second


def shuffle_lanes(pairs):
    lane = lax.broadcasted_iota(jnp.int32, (8, 128), 1) < 64
    return [exchange(a, b, 64, lane) for a, b in pairs]


def shuffle_rows(four):
    row = lax.broadcasted_iota(jnp.int32, (8, 128), 0)
    top, even = row < 4, row % 4 < 2
    a0, b0 = exchange(four[0], four[2], 4, top)
    a1, b1 = exchange(four[1], four[3], 4, top)
    c0, c1 = exchange(a0, a1, 2, even)
    c2, c3 = exchange(b0, b1, 2, even)
    return [c0, c1, c2, c3]


def pack(read, write):
    pairs = shuffle_lanes([(read(z, 0), read(z, 1)) for z in range(PLANES)])
    for qb in range(2):
        for inner, chunk in enumerate(shuffle_rows([pairs[z][qb] for z in range(PLANES)])):
            write(inner, qb, chunk)


def unpack(read, write):
    columns = [shuffle_rows([read(inner, qb) for inner in range(4)]) for qb in range(2)]
    for z in range(PLANES):
        ((first, second),) = shuffle_lanes([(columns[0][z], columns[1][z])])
        write(z, 0, first)
        write(z, 1, second)


def cubic(u, strength):
    return REACT * strength * (u - u * u * u)


def first_kernel(
    node, u_far, k_far, x_far, y_far, out_ref, rows, part, u_near, k_near, x_near, y_near, sems
):
    me = node[0]
    copies = [pltpu.make_async_copy(y_far.at[me], y_near, sems.at[0])]
    for z in range(PLANES):
        copies.append(pltpu.make_async_copy(u_far.at[z], u_near.at[z], sems.at[2 * z + 1]))
        copies.append(pltpu.make_async_copy(k_far.at[z], k_near.at[z], sems.at[2 * z + 2]))
    copies.append(pltpu.make_async_copy(x_far, x_near, sems.at[9]))
    for copy in copies:
        copy.start()
    copies[0].wait()
    for z in range(PLANES):
        copies[2 * z + 1].wait()
        copies[2 * z + 2].wait()
        u = u_near[z]
        for array, field in enumerate((u, cubic(u, k_near[z]))):
            a, b = split(field)
            part[array, z] = product(y_near[...], jnp.concatenate([a, b, a], axis=0))
    copies[9].wait()
    for array in range(2):
        whole_part = times(part[array].reshape(PLANES * 32, NXY), x_near)
        rows[array] = whole_part.reshape(PLANES, 2, 16, NXY)
    for array in range(2):
        for g in range(2):
            for hq in range(2):
                lanes = slice(hq * 128, hq * 128 + 128)

                def read(z, b):
                    return rows[array, z, b, g * 8 : g * 8 + 8, lanes]

                def write(inner, qb, chunk):
                    out_ref[g, hq, inner, qb, array] = chunk

                pack(read, write)


def gather_rows(in_ref, rows):
    for kg in range(16):
        for hq in range(2):
            lanes = slice(hq * 128, hq * 128 + 128)

            def read(inner, qb):
                return in_ref[kg, hq, inner, qb]

            def write(z, b, tile):
                rows[z, b, kg * 8 : kg * 8 + 8, lanes] = tile

            unpack(read, write)


def scatter_rows(rows, out_ref):
    for kg in range(16):
        for hq in range(2):
            lanes = slice(hq * 128, hq * 128 + 128)

            def read(z, b):
                return rows[z, b, kg * 8 : kg * 8 + 8, lanes]

            def write(inner, qb, chunk):
                out_ref[kg, hq, inner, qb] = chunk

            pack(read, write)


def middle_kernel(in_ref, k_ref, x_fwd, x_inv, y_fwd, y_inv, out_ref, rows, part):
    gather_rows(in_ref, rows)
    for z in range(PLANES):
        part[z] = apply(y_inv, rows[z].reshape(NXY, NXY))
    for z in range(PLANES):
        part[z] = cubic(times(part[z], x_inv), k_ref[z])
    for z in range(PLANES):
        part[z] = times(part[z], x_fwd)
    for z in range(PLANES):
        rows[z] = apply(y_fwd, part[z]).reshape(2, 128, NXY)
    scatter_rows(rows, out_ref)


def last_kernel(in_ref, x_inv, y_inv, out_far, rows, part, sems):
    gather_rows(in_ref, rows)
    for z in range(PLANES):
        part[z] = apply(y_inv, rows[z].reshape(NXY, NXY))
    copies = []
    for z in range(PLANES):
        part[z] = times(part[z], x_inv)
        copies.append(pltpu.make_async_copy(part.at[z], out_far.at[0, z], sems.at[z]))
        copies[z].start()
    for copy in copies:
        copy.wait()


def lane_pair(value, distance, upper):
    if distance == 64:
        return value + pltpu.roll(value, 64, value.ndim - 1)
    ahead = pltpu.roll(value, 128 - distance, value.ndim - 1)
    behind = pltpu.roll(value, distance, value.ndim - 1)
    return value + jnp.where(upper, behind, ahead)


def mode_tables(group, zlev0, zlev1, zlev2, ytable, xtable):
    tile = pl.ds(group * 8, 8)

    def row(i, join):
        return jnp.broadcast_to(join(ytable[0, i : i + 1], xtable[0, i : i + 1]), (8, 128))

    total = [row(i, jnp.add) for i in (0, 1, 4, 6)]
    scale = [row(i, jnp.multiply) for i in (2, 3, 5)]
    ring0 = [[[zlev0[0, c, d, tile] + total[a] for d in range(2)] for c in range(2)] for a in range(2)]
    mean0 = [[[zlev0[1, c, d, tile] * scale[a] for d in range(2)] for c in range(2)] for a in range(2)]
    ring1 = [zlev1[0, d, tile] + total[2] for d in range(2)]
    mean1 = [zlev1[1, d, tile] * scale[2] for d in range(2)]
    ring2 = zlev2[tile] + total[3]
    three = lambda v: jnp.stack([jnp.stack([jnp.stack(y) for y in x]) for x in v])
    return three(ring0), three(mean0), jnp.stack(ring1), jnp.stack(mean1), ring2


def write_weights(shifts, tables, tile, weights):
    quad, rise, spread, keep, send, down1, gain1, back1 = weights
    ring0, mean0, ring1, mean1, ring2 = tables
    for m, s in enumerate(shifts):
        s1, s2 = s / 4.0, s / 16.0
        weight = OMEGA / (1.0 + 6.0 * s)
        weight1, weight2 = OMEGA / (1.0 + 6.0 * s1), OMEGA / (1.0 + 6.0 * s2)
        sigma = (1.0 - OMEGA) + (weight * s) * ring0
        square = sigma * sigma
        lower = mean0 * square
        quad[m, :, :, :, tile] = square * square
        rise[m, :, :, :, tile] = weight * (square + 1.0) * (sigma + 1.0)
        spread[m, :, :, :, tile] = 8.0 * lower
        keep[m, :, :, :, tile] = lower * (sigma - 1.0)
        send[m, :, :, :, tile] = weight * lower
        sigma1 = (1.0 - OMEGA) + (weight1 * s1) * ring1
        sigma2 = (1.0 - OMEGA) + (weight2 * s2) * ring2
        square1 = sigma1 * sigma1
        square2 = sigma2 * sigma2
        sweeps = (1.0 + sigma2) * (1.0 + square2) * (1.0 + square2 * square2)
        down1[m, :, tile] = (weight1 / weight) * (mean1 * square1)
        gain1[m, :, tile] = (weight1 / weight) * (1.0 + sigma1) * (1.0 + square1)
        back1[m, :, tile] = (8.0 * weight2 / weight1) * (mean1 * square1 * sweeps)


def vcycles(tile, weights, v, base, down):
    quad, rise, spread, keep, send, down1, gain1, back1 = weights
    lane = lax.broadcasted_iota(jnp.int32, (2, 8, 128), 2)
    upper32 = lane % 64 >= 32
    upper16 = (lane % 32 >= 16)[0]
    at = lambda ref, m: ref[m, :, :, :, tile]
    for cycle in range(VCYCLES):
        sums = []
        for m in range(NODES):
            remain = at(keep, m) * v[m] + down[m]
            sums.append((remain[0, 0] + remain[0, 1]) + (remain[1, 0] + remain[1, 1]))
        corrections = []
        for m in range(NODES):
            source1 = lane_pair(sums[m], 32, upper32)
            lower = down1[m, :, tile] * source1
            total = lane_pair(lane_pair(lower[0] + lower[1], 64, None), 16, upper16)
            corrections.append(gain1[m, :, tile] * source1 + back1[m, :, tile] * total)
        for m in range(NODES):
            v[m] = at(quad, m) * v[m] + base[m] + at(spread, m) * corrections[m]


def laplacian(zlev0, tile, ytable, xtable):
    near = [
        jnp.broadcast_to(ytable[0, a : a + 1] + xtable[0, a : a + 1] - 6.0, (8, 128))
        for a in range(2)
    ]
    line = zlev0[0, :, :, tile]
    return jnp.stack([line + near[a] for a in range(2)])


def to_slabs(modes, z_inv, out_ref):
    for pair in range(NODES // 2):
        both = jnp.concatenate(
            [modes[2 * pair + i].reshape(2 * NZ, 128) for i in range(2)], axis=1
        )
        both = apply(z_inv, both)
        for i in range(2):
            out_ref[2 * pair + i] = both[:, i * 128 : i * 128 + 128].reshape(SLABS, 8, 128)


def start_kernel(
    shifts, sums, place, in_ref, z_fwd, z_inv, zlev0, zlev1, zlev2, ytable, xtable,
    out_ref, sections, start, quad, rise, spread, keep, send, down1, gain1, back1, cubes, v, base, down,
):
    both = jnp.concatenate([in_ref[:, i].reshape(2 * NZ, 128) for i in range(2)], axis=1)
    both = apply(z_fwd, both)
    start[...] = both[:, :128].reshape(2, 2, 2, 32, 128)
    cubes[...] = both[:, 128:].reshape(2, 2, 2, 32, 128)

    def group_step(group, carry):
        tile = pl.ds(group * 8, 8)
        tables = mode_tables(group, zlev0, zlev1, zlev2, ytable, xtable)
        weights = (quad, rise, spread, keep, send, down1, gain1, back1)
        write_weights(shifts, tables, tile, weights)
        lap = tables[0] - 6.0
        u = start[:, :, :, tile]
        cube = cubes[:, :, :, tile]
        for m, s in enumerate(shifts):
            right = (1.0 + (DIFFUSE * sums[m] - s) * lap) * u + sums[m] * cube
            base[m] = rise[m, :, :, :, tile] * right
            down[m] = send[m, :, :, :, tile] * right
            v[m] = u
        vcycles(tile, weights, v, base, down)
        for m in range(NODES):
            sections[m, :, :, :, tile] = v[m]
        return carry

    lax.fori_loop(0, 4, group_step, 0)
    to_slabs(sections, z_inv, out_ref)


def step_kernel(
    shifts, quadrature, place, in_ref, sections, start, z_fwd, z_inv, zlev0, quad, rise, spread, keep,
    send, down1, gain1, back1, ytable, xtable, out_ref, cubes, force, v, base, down,
):
    for pair in range(NODES // 2):
        both = jnp.concatenate(
            [in_ref[2 * pair + i].reshape(2 * NZ, 128) for i in range(2)], axis=1
        )
        both = apply(z_fwd, both)
        for i in range(2):
            part = both[:, i * 128 : i * 128 + 128]
            cubes[2 * pair + i] = part.reshape(2, 2, 2, 32, 128)

    def group_step(group, carry):
        tile = pl.ds(group * 8, 8)
        lap = laplacian(zlev0, tile, ytable, xtable)
        double = DIFFUSE * lap
        for m in range(NODES):
            force[m] = double * sections[m, :, :, :, tile] + cubes[m, :, :, :, tile]
        for m, s in enumerate(shifts):
            u = sections[m, :, :, :, tile]
            right = start[:, :, :, tile] - s * (lap * u)
            for j in range(NODES):
                right = right + quadrature[m][j] * force[j]
            base[m] = rise[m, :, :, :, tile] * right
            down[m] = send[m, :, :, :, tile] * right
            v[m] = u
        vcycles(tile, (quad, rise, spread, keep, send, down1, gain1, back1), v, base, down)
        for m in range(NODES):
            cubes[m, :, :, :, tile] = v[m]
        return carry

    lax.fori_loop(0, 4, group_step, 0)
    to_slabs(cubes, z_inv, out_ref)


def whole(shape):
    return pl.BlockSpec(shape, lambda *_: (0,) * len(shape))


FAR = pl.BlockSpec(memory_space=pltpu.MemorySpace.HBM)


def run(kernel, args, outs, scratch, scalar=None, tables=(), far=False, far_out=False):
    specs = [FAR if far else whole(a.shape) for a in args]
    if tables:
        base = lambda i, place: (place[0] // 16 * 4 + place[0] // 2 % 4, 0, 0)
        part = lambda i, place: (place[0] // 8 % 2 * 2 + place[0] % 2, 0, 0)
        specs += [pl.BlockSpec((1, 8, 128), base), pl.BlockSpec((1, 8, 128), part)]
    out_shape = [jax.ShapeDtypeStruct(shape, jnp.float32) for shape in outs]
    out_specs = [FAR if far_out else whole(shape) for shape in outs]
    grid_spec = pltpu.PrefetchScalarGridSpec(
        num_scalar_prefetch=0 if scalar is None else 1,
        grid=(1,),
        in_specs=specs,
        out_specs=out_specs,
        scratch_shapes=[pltpu.VMEM(s, jnp.float32) if isinstance(s, tuple) else s for s in scratch],
    )
    call = pl.pallas_call(
        kernel,
        grid_spec=grid_spec,
        out_shape=out_shape,
        compiler_params=pltpu.CompilerParams(vmem_limit_bytes=40 * 1024 * 1024),
    )
    if far:
        args = [pltpu.with_memory_space_constraint(a, pltpu.MemorySpace.HBM) for a in args]
    return call(*([] if scalar is None else [scalar]), *args, *tables)


def per_device(initial, kappa):
    abscissa, quadrature = radau_table(NODES)
    shifts = [DIFFUSE * value for value in abscissa]
    sums = [sum(row) for row in quadrature]
    c = {name: jnp.asarray(value) for name, value in constants().items()}
    node = lax.axis_index("node")
    place = (node * SLABS + lax.axis_index("space")).astype(jnp.int32).reshape(1)
    node = node.astype(jnp.int32).reshape(1)
    levels = (c["zlev0"], c["zlev1"], c["zlev2"])
    rows = (PLANES, 2, 128, NXY)
    tile = (2, 2, 2, 8, 128)
    modes = (2, 2, 2, 32, 128)

    (sent,) = run(
        first_kernel,
        (initial, kappa, c["x_fwd"], c["y_first"]),
        [(2, 2, 4, 2, 2, 8, 128)],
        [
            (2, PLANES, 2, 16, NXY),
            (2, PLANES, 32, NXY),
            (PLANES, NXY, NXY),
            (PLANES, NXY, NXY),
            pltpu.VMEM((2, NXY, NXY), jnp.bfloat16),
            pltpu.VMEM((32, 3 * NXY), jnp.bfloat16),
            pltpu.SemaphoreType.DMA((10,)),
        ],
        scalar=node,
        far=True,
    )
    tables = (c["ytable"], c["xtable"])
    half = (2, 32, 128)
    held = lax.all_to_all(sent.reshape(SLABS, 2, 8, 128), "space", 0, 0, tiled=True)
    sent, sections, start, *weights = run(
        functools.partial(start_kernel, shifts, sums),
        (held, c["z_fwd"], c["z_inv"], *levels),
        [(NODES, SLABS, 8, 128), (NODES,) + modes, modes]
        + [(NODES,) + modes] * 5
        + [(NODES,) + half] * 3,
        [modes] + [(NODES,) + tile] * 3,
        scalar=place,
        tables=tables,
    )
    both = ("node", "space")
    count = NODES * SLABS
    held = lax.all_to_all(sent.reshape(count, 8, 128), both, 0, 0, tiled=True)
    (sent,) = run(
        middle_kernel,
        (held.reshape(16, 2, 4, 2, 8, 128), kappa, c["x_fwd"], c["x_inv"], c["y_fwd"], c["y_inv"]),
        [(16, 2, 4, 2, 8, 128)],
        [rows, (PLANES, NXY, NXY)],
    )
    held = lax.all_to_all(sent.reshape(count, 8, 128), both, 0, 0, tiled=True)
    (sent,) = run(
        functools.partial(step_kernel, shifts, quadrature),
        (held.reshape(NODES, SLABS, 8, 128), sections, start, c["z_fwd"], c["z_inv"], c["zlev0"], *weights),
        [(NODES, SLABS, 8, 128)],
        [(NODES,) + modes] + [(NODES,) + tile] * 4,
        scalar=place,
        tables=tables,
    )
    held = lax.all_to_all(sent.reshape(count, 8, 128), both, 0, 0, tiled=True)
    (out,) = run(
        last_kernel,
        (held.reshape(16, 2, 4, 2, 8, 128), c["x_inv"], c["y_inv"]),
        [(1, PLANES, NXY, NXY)],
        [rows, (PLANES, NXY, NXY), pltpu.SemaphoreType.DMA((PLANES,))],
        far_out=True,
    )
    return out


def solution(mesh):
    in_specs = (P("space", None, None), P("space", None, None))
    out_specs = P("node", "space", None, None)
    return jax.shard_map(
        per_device, mesh=mesh, in_specs=in_specs, out_specs=out_specs, check_vma=False
    )
```

```python
import functools

import jax
import jax.numpy as jnp
import ml_dtypes
import numpy as np
from jax import lax
from jax.experimental import pallas as pl
from jax.experimental.pallas import tpu as pltpu
from jax.sharding import PartitionSpec as P

DIFFUSE = 2.0
REACT = 0.5
OMEGA = 0.8
NODES = 8
SLABS = 32
PLANES = 4
NZ = 128
NXY = 256
VCYCLES = 2


def radau_gap(count, where):
    previous = 1.0
    current = where
    for degree in range(1, count):
        following = ((2 * degree + 1) * where * current - degree * previous) / (degree + 1)
        previous = current
        current = following
    return current - previous


def radau_table(count):
    zeros_found = []
    grid_count = 4096
    lower = -1.0
    value_low = radau_gap(count, lower)
    for place in range(1, grid_count):
        upper = -1.0 + 2.0 * place / grid_count
        value_up = radau_gap(count, upper)
        if value_low * value_up < 0.0:
            left_end = lower
            right_end = upper
            left_value = value_low
            for halving in range(100):
                middle = 0.5 * (left_end + right_end)
                middle_value = radau_gap(count, middle)
                if left_value * middle_value <= 0.0:
                    right_end = middle
                else:
                    left_end = middle
                    left_value = middle_value
            zeros_found.append(0.5 * (left_end + right_end))
        lower = upper
        value_low = value_up
    zeros_found.append(1.0)
    abscissa = [(value + 1.0) / 2.0 for value in zeros_found]
    table_rows = []
    for outer in range(count):
        table_rows.append([0.0] * count)
    for column in range(count):
        factor = [1.0]
        scale = 1.0
        for other in range(count):
            if other != column:
                widened = [0.0] * (len(factor) + 1)
                for power in range(len(factor)):
                    widened[power + 1] = widened[power + 1] + factor[power]
                    widened[power] = widened[power] - abscissa[other] * factor[power]
                factor = widened
                scale = scale * (abscissa[column] - abscissa[other])
        for outer in range(count):
            upto = abscissa[outer]
            accum = 0.0
            for power in range(len(factor)):
                accum = accum + factor[power] * upto ** (power + 1) / (power + 1)
            table_rows[outer][column] = accum / scale
    return (abscissa, table_rows)


def mode_list(n):
    return [("c", k) for k in range(n // 2)] + [("s", k) for k in range(1, n // 2 + 1)]


def mode_vector(n, kind, k):
    angle = 2.0 * np.pi * k * (np.arange(n) + 0.5) / n
    values = np.cos(angle) if kind == "c" else np.sin(angle)
    return values / np.sqrt((values * values).sum())


def child_mode(coarse, kind, k, which):
    if which == 0:
        return (kind, k)
    if kind == "c":
        return ("s", coarse) if k == 0 else ("c", coarse - k)
    return ("c", coarse // 2) if k == coarse // 2 else ("s", coarse - k)


def pair_mean(n):
    return np.kron(np.eye(n // 2), np.full((1, 2), 0.5))


def dimension_tables(n):
    mid, low = n // 2, n // 4
    basis = np.zeros((2, 2, low, n))
    basis1 = np.zeros((2, low, mid))
    basis2 = np.zeros((low, low))
    ring0, ring1, ring2 = np.zeros((2, 2, low)), np.zeros((2, low)), np.zeros(low)
    for i, (kind, k) in enumerate(mode_list(low)):
        basis2[i] = mode_vector(low, kind, k)
        ring2[i] = 2.0 * np.cos(2.0 * np.pi * k / low)
        for b in range(2):
            kind1, k1 = child_mode(low, kind, k, b)
            basis1[b, i] = mode_vector(mid, kind1, k1)
            ring1[b, i] = 2.0 * np.cos(2.0 * np.pi * k1 / mid)
            for a in range(2):
                kind0, k0 = child_mode(mid, kind1, k1, a)
                basis[a, b, i] = mode_vector(n, kind0, k0)
                ring0[a, b, i] = 2.0 * np.cos(2.0 * np.pi * k0 / n)
    mean0 = np.einsum("bin,abin->abi", basis1 @ pair_mean(n), basis)
    mean1 = np.einsum("in,bin->bi", basis2 @ pair_mean(mid), basis1)
    return basis, ring0, mean0, ring1, mean1, ring2


def halves(matrix):
    high = matrix.astype(ml_dtypes.bfloat16)
    rest = (matrix - high.astype(np.float64)).astype(ml_dtypes.bfloat16)
    return np.stack([high, rest])


@functools.lru_cache(maxsize=None)
def constants():
    basis, ring0, mean0, ring1, mean1, ring2 = dimension_tables(NXY)
    low = NXY // 4
    to_x = basis.reshape(2, 2, 2, 2, 16, NXY).transpose(2, 0, 3, 1, 4, 5).reshape(NXY, NXY)
    to_y = basis.transpose(1, 2, 0, 3).reshape(NXY, NXY)
    first_y = basis.transpose(1, 2, 0, 3).reshape(2, NODES, 16, NXY)
    first_y = first_y.transpose(1, 0, 2, 3).reshape(NODES, 32, NXY)

    zbasis, zring0, zmean0, zring1, zmean1, zring2 = dimension_tables(NZ)
    along = zbasis.reshape(NZ, SLABS, PLANES)
    to_z = np.einsum("ac,kgisz->gakiszc", np.eye(2), along.reshape(4, 4, 8, SLABS, PLANES))
    to_z = to_z.reshape(2 * NZ, 2 * NZ)

    wide = lambda v: np.repeat(v[..., None], 128, axis=-1)
    grouped = lambda v: np.moveaxis(v.reshape(v.shape[:-1] + (4, 8)), -2, 0)
    zlev0 = wide(np.stack([grouped(zring0), grouped(zmean0)]))
    zlev1 = wide(np.stack([grouped(zring1), grouped(zmean1)]))
    zlev2 = wide(grouped(zring2))

    lanes = lambda v: np.broadcast_to(v, v.shape[:-4] + (2, 2, 2, 16)).reshape(v.shape[:-4] + (128,))
    ytable = np.zeros((low, 8, 128))
    for base in range(low):
        over_b = lambda v: lanes(v[:, base].reshape(1, 2, 1, 1))
        for a in range(2):
            ytable[base, a] = over_b(ring0[a])
            ytable[base, 2 + a] = over_b(mean0[a])
        ytable[base, 4] = over_b(ring1)
        ytable[base, 5] = over_b(mean1)
        ytable[base, 6] = ring2[base]
    xtable = np.zeros((4, 8, 128))
    for q in range(4):
        xs = slice(q * 16, q * 16 + 16)
        for a in range(2):
            xtable[q, a] = lanes(ring0[:, None, :, xs])
            xtable[q, 2 + a] = lanes(mean0[:, None, :, xs])
        xtable[q, 4] = lanes(ring1[None, None, :, xs])
        xtable[q, 5] = lanes(mean1[None, None, :, xs])
        xtable[q, 6] = lanes(ring2[None, None, None, xs])
    f32 = lambda v: np.asarray(v, np.float32)
    return {
        "x_fwd": halves(to_x.T.copy()),
        "x_inv": halves(to_x),
        "y_fwd": halves(to_y),
        "y_inv": halves(to_y.T.copy()),
        "y_first": np.concatenate([halves(first_y)[i] for i in (0, 0, 1)], axis=2),
        "z_fwd": halves(to_z),
        "z_inv": halves(to_z.T.copy()),
        "zlev0": f32(zlev0),
        "zlev1": f32(zlev1),
        "zlev2": f32(zlev2),
        "ytable": f32(ytable),
        "xtable": f32(xtable),
    }


def split(value):
    high = value.astype(jnp.bfloat16)
    return high, (value - high.astype(jnp.float32)).astype(jnp.bfloat16)


def product(a, b):
    return jnp.dot(a, b, preferred_element_type=jnp.float32)


def times(left, matrix):
    a, b = split(left)
    return product(
        jnp.concatenate([a, b, a], axis=1),
        jnp.concatenate([matrix[0], matrix[0], matrix[1]], axis=0),
    )


def apply(matrix, right):
    a, b = split(right)
    return product(
        jnp.concatenate([matrix[0], matrix[0], matrix[1]], axis=1),
        jnp.concatenate([a, b, a], axis=0),
    )


def exchange(low, high, shift, keep):
    size = low.shape[0 if shift < 8 else 1]
    axis = 0 if shift < 8 else 1
    first = jnp.where(keep, low, pltpu.roll(high, shift, axis))
    second = jnp.where(keep, pltpu.roll(low, size - shift, axis), high)
    return first, second


def shuffle_lanes(pairs):
    keep = lax.broadcasted_iota(jnp.int32, (8, 128), 1) % 64 < 32
    return [exchange(a, b, 32, keep) for a, b in pairs]


def shuffle_rows(four):
    row = lax.broadcasted_iota(jnp.int32, (8, 128), 0)
    top, even = row < 4, row % 4 < 2
    a0, b0 = exchange(four[0], four[2], 4, top)
    a1, b1 = exchange(four[1], four[3], 4, top)
    c0, c1 = exchange(a0, a1, 2, even)
    c2, c3 = exchange(b0, b1, 2, even)
    return [c0, c1, c2, c3]


def pack(read, write):
    pairs = shuffle_lanes([(read(z, 0), read(z, 1)) for z in range(PLANES)])
    for qb in range(2):
        for inner, chunk in enumerate(shuffle_rows([pairs[z][qb] for z in range(PLANES)])):
            write(inner, qb, chunk)


def unpack(read, write):
    columns = [shuffle_rows([read(inner, qb) for inner in range(4)]) for qb in range(2)]
    for z in range(PLANES):
        ((first, second),) = shuffle_lanes([(columns[0][z], columns[1][z])])
        write(z, 0, first)
        write(z, 1, second)


def cubic(u, strength):
    return REACT * strength * (u - u * u * u)


def first_kernel(
    place, u_far, k_far, x_far, y_far, out_ref, rows, part, u_near, k_near, x_near, y_near, sems
):
    me = place[0] // SLABS
    copies = [pltpu.make_async_copy(y_far.at[me], y_near, sems.at[0])]
    for z in range(PLANES):
        copies.append(pltpu.make_async_copy(u_far.at[z], u_near.at[z], sems.at[2 * z + 1]))
        copies.append(pltpu.make_async_copy(k_far.at[z], k_near.at[z], sems.at[2 * z + 2]))
    copies.append(pltpu.make_async_copy(x_far, x_near, sems.at[9]))
    for copy in copies:
        copy.start()
    copies[0].wait()
    for z in range(PLANES):
        copies[2 * z + 1].wait()
        copies[2 * z + 2].wait()
        u = u_near[z]
        for array, field in enumerate((u, cubic(u, k_near[z]))):
            a, b = split(field)
            part[array, z] = product(y_near[...], jnp.concatenate([a, b, a], axis=0))
    copies[9].wait()
    for array in range(2):
        whole_part = times(part[array].reshape(PLANES * 32, NXY), x_near)
        rows[array] = whole_part.reshape(PLANES, 2, 16, NXY)
    for array in range(2):
        for g in range(2):
            for hq in range(2):
                lanes = slice(hq * 128, hq * 128 + 128)

                def read(z, b):
                    return rows[array, z, b, g * 8 : g * 8 + 8, lanes]

                def write(inner, qb, chunk):
                    out_ref[g, hq, inner, qb, array] = chunk

                pack(read, write)


def gather_rows(in_ref, rows):
    for kg in range(16):
        for hq in range(2):
            lanes = slice(hq * 128, hq * 128 + 128)

            def read(inner, qb):
                return in_ref[kg, hq, inner, qb]

            def write(z, b, tile):
                rows[z, b, kg * 8 : kg * 8 + 8, lanes] = tile

            unpack(read, write)


def scatter_rows(rows, out_ref):
    for kg in range(16):
        for hq in range(2):
            lanes = slice(hq * 128, hq * 128 + 128)

            def read(z, b):
                return rows[z, b, kg * 8 : kg * 8 + 8, lanes]

            def write(inner, qb, chunk):
                out_ref[kg, hq, inner, qb] = chunk

            pack(read, write)


def middle_kernel(in_ref, k_ref, x_fwd, x_inv, y_fwd, y_inv, out_ref, rows, part):
    gather_rows(in_ref, rows)
    for z in range(PLANES):
        part[z] = apply(y_inv, rows[z].reshape(NXY, NXY))
    for z in range(PLANES):
        part[z] = cubic(times(part[z], x_inv), k_ref[z])
    for z in range(PLANES):
        part[z] = times(part[z], x_fwd)
    for z in range(PLANES):
        rows[z] = apply(y_fwd, part[z]).reshape(2, 128, NXY)
    scatter_rows(rows, out_ref)


def last_kernel(in_ref, x_inv, y_inv, out_far, rows, part, sems):
    gather_rows(in_ref, rows)
    for z in range(PLANES):
        part[z] = apply(y_inv, rows[z].reshape(NXY, NXY))
    copies = []
    for z in range(PLANES):
        part[z] = times(part[z], x_inv)
        copies.append(pltpu.make_async_copy(part.at[z], out_far.at[0, z], sems.at[z]))
        copies[z].start()
    for copy in copies:
        copy.wait()


def lane_pair(value, distance):
    return value + pltpu.roll(value, distance, value.ndim - 1)


def mode_tables(group, zlev0, zlev1, zlev2, ytable, xtable):

    def row(i, join):
        return jnp.broadcast_to(join(ytable[0, i : i + 1], xtable[0, i : i + 1]), (8, 128))

    total = [row(i, jnp.add) for i in (0, 1, 4, 6)]
    scale = [row(i, jnp.multiply) for i in (2, 3, 5)]
    ring0 = [[[zlev0[0, group, c, d] + total[a] for d in range(2)] for c in range(2)] for a in range(2)]
    mean0 = [[[zlev0[1, group, c, d] * scale[a] for d in range(2)] for c in range(2)] for a in range(2)]
    ring1 = [zlev1[0, group, d] + total[2] for d in range(2)]
    mean1 = [zlev1[1, group, d] * scale[2] for d in range(2)]
    ring2 = zlev2[group] + total[3]
    three = lambda v: jnp.stack([jnp.stack([jnp.stack(y) for y in x]) for x in v])
    return three(ring0), three(mean0), jnp.stack(ring1), jnp.stack(mean1), ring2


def write_weights(shifts, tables, group, weights):
    quad, rise, lower, keep, down1, gain1, back1 = weights
    ring0, mean0, ring1, mean1, ring2 = tables
    for m, s in enumerate(shifts):
        s1, s2 = s / 4.0, s / 16.0
        weight = OMEGA / (1.0 + 6.0 * s)
        weight1, weight2 = OMEGA / (1.0 + 6.0 * s1), OMEGA / (1.0 + 6.0 * s2)
        sigma = (1.0 - OMEGA) + (weight * s) * ring0
        square = sigma * sigma
        scaled = mean0 * square
        quad[m, group] = square * square
        rise[m, group] = (square + 1.0) * (sigma + 1.0)
        lower[m, group] = scaled
        keep[m, group] = scaled * (sigma - 1.0)
        sigma1 = (1.0 - OMEGA) + (weight1 * s1) * ring1
        sigma2 = (1.0 - OMEGA) + (weight2 * s2) * ring2
        square1 = sigma1 * sigma1
        square2 = sigma2 * sigma2
        sweeps = (1.0 + sigma2) * (1.0 + square2) * ((64.0 * weight2 / weight1) * (1.0 + square2 * square2))
        passed = mean1 * square1
        down1[m, group] = (weight1 / weight) * passed
        gain1[m, group] = (8.0 * weight1 / weight) * ((1.0 + sigma1) * (1.0 + square1))
        back1[m, group] = passed * sweeps


def pair_sums(m, group, v, weights, down, sums):
    keep = weights[3]
    remain = keep[m, group] * v + down
    sums[m, group] = (remain[0, 0] + remain[0, 1]) + (remain[1, 0] + remain[1, 1])


def correct(weights, sums):
    down1, gain1, back1 = weights[4:]
    for m in range(NODES):
        source1 = lane_pair(sums[m], 64)
        lower = down1[m] * source1
        total = lane_pair(lane_pair(lower[:, 0] + lower[:, 1], 32), 16)
        sums[m] = gain1[m] * source1 + back1[m] * total[:, None]


def finish_cycles(weights, first, v, base, down, sums):
    quad, lower = weights[0], weights[2]
    for cycle in range(VCYCLES):
        before = first if cycle == 0 else v
        correct(weights, sums)

        def group_step(group, carry):
            for m in range(NODES):
                field = quad[m, group] * before[m, group] + base[m, group]
                field = field + lower[m, group] * sums[m, group]
                v[m, group] = field
                if cycle + 1 < VCYCLES:
                    pair_sums(m, group, field, weights, down[m, group], sums)
            return carry

        lax.fori_loop(0, 4, group_step, 0)


def place_rows(place, ytable, xtable):
    base = place // 16 * 4 + place // 2 % 4
    part = place // 8 % 2 * 2 + place % 2
    return ytable.at[pl.ds(base, 1)], xtable.at[pl.ds(part, 1)]


def laplacian(zlev0, group, ytable, xtable):
    near = [
        jnp.broadcast_to(ytable[0, a : a + 1] + xtable[0, a : a + 1] - 6.0, (8, 128))
        for a in range(2)
    ]
    line = zlev0[0, group]
    return jnp.stack([line + near[a] for a in range(2)])


def to_slabs(modes, z_inv, out_ref):
    for pair in range(NODES // 2):
        both = jnp.concatenate(
            [modes[2 * pair + i].reshape(2 * NZ, 128) for i in range(2)], axis=1
        )
        both = apply(z_inv, both)
        for i in range(2):
            out_ref[2 * pair + i] = both[:, i * 128 : i * 128 + 128].reshape(SLABS, 8, 128)


def start_kernel(
    shifts, sums, place, in_ref, z_fwd, z_inv, zlev0, zlev1, zlev2, ytable, xtable,
    out_ref, sections, start, quad, rise, lower, keep, down1, gain1, back1,
    cubes, base, down, pairs,
):
    weights = (quad, rise, lower, keep, down1, gain1, back1)
    ytable, xtable = place_rows(place[0], ytable, xtable)
    both = jnp.concatenate([in_ref[:, i].reshape(2 * NZ, 128) for i in range(2)], axis=1)
    both = apply(z_fwd, both)
    start[...] = both[:, :128].reshape(4, 2, 2, 2, 8, 128)
    cubes[...] = both[:, 128:].reshape(4, 2, 2, 2, 8, 128)

    def group_step(group, carry):
        tables = mode_tables(group, zlev0, zlev1, zlev2, ytable, xtable)
        write_weights(shifts, tables, group, weights)
        lap = tables[0] - 6.0
        u = start[group]
        cube = cubes[group]
        for m, s in enumerate(shifts):
            weight = OMEGA / (1.0 + 6.0 * s)
            source = (weight + (weight * (DIFFUSE * sums[m] - s)) * lap) * u + (weight * sums[m]) * cube
            base[m, group] = rise[m, group] * source
            passed = lower[m, group] * source
            down[m, group] = passed
            sections[m, group] = u
            pair_sums(m, group, u, weights, passed, pairs)
        return carry

    lax.fori_loop(0, 4, group_step, 0)
    finish_cycles(weights, sections, sections, base, down, pairs)
    to_slabs(sections, z_inv, out_ref)


def step_kernel(
    shifts, quadrature, place, in_ref, sections, start, z_fwd, z_inv, zlev0, quad, rise, lower, keep,
    down1, gain1, back1, ytable, xtable, out_ref, cubes, force, base, down, pairs,
):
    weights = (quad, rise, lower, keep, down1, gain1, back1)
    ytable, xtable = place_rows(place[0], ytable, xtable)
    for pair in range(NODES // 2):
        both = jnp.concatenate(
            [in_ref[2 * pair + i].reshape(2 * NZ, 128) for i in range(2)], axis=1
        )
        both = apply(z_fwd, both)
        for i in range(2):
            part = both[:, i * 128 : i * 128 + 128]
            cubes[2 * pair + i] = part.reshape(4, 2, 2, 2, 8, 128)

    def group_step(group, carry):
        lap = laplacian(zlev0, group, ytable, xtable)
        double = DIFFUSE * lap
        for m in range(NODES):
            force[m] = double * sections[m, group] + cubes[m, group]
        for m, s in enumerate(shifts):
            u = sections[m, group]
            weight = OMEGA / (1.0 + 6.0 * s)
            source = weight * start[group] - (weight * s) * (lap * u)
            for j in range(NODES):
                source = source + (weight * quadrature[m][j]) * force[j]
            base[m, group] = rise[m, group] * source
            passed = lower[m, group] * source
            down[m, group] = passed
            pair_sums(m, group, u, weights, passed, pairs)
        return carry

    lax.fori_loop(0, 4, group_step, 0)
    finish_cycles(weights, sections, cubes, base, down, pairs)
    to_slabs(cubes, z_inv, out_ref)


def whole(shape):
    return pl.BlockSpec(shape, lambda *_: (0,) * len(shape))


FAR = pl.BlockSpec(memory_space=pltpu.MemorySpace.HBM)


def run(kernel, args, outs, scratch, scalar=None, far=False, far_out=False):
    specs = [FAR if far else whole(a.shape) for a in args]
    out_shape = [jax.ShapeDtypeStruct(shape, jnp.float32) for shape in outs]
    out_specs = [FAR if far_out else whole(shape) for shape in outs]
    grid_spec = pltpu.PrefetchScalarGridSpec(
        num_scalar_prefetch=0 if scalar is None else 1,
        grid=(1,),
        in_specs=specs,
        out_specs=out_specs,
        scratch_shapes=[pltpu.VMEM(s, jnp.float32) if isinstance(s, tuple) else s for s in scratch],
    )
    call = pl.pallas_call(
        kernel,
        grid_spec=grid_spec,
        out_shape=out_shape,
        compiler_params=pltpu.CompilerParams(vmem_limit_bytes=40 * 1024 * 1024),
    )
    if far:
        args = [pltpu.with_memory_space_constraint(a, pltpu.MemorySpace.HBM) for a in args]
    return call(*([] if scalar is None else [scalar]), *args)


def per_device(initial, kappa):
    abscissa, quadrature = radau_table(NODES)
    shifts = [DIFFUSE * value for value in abscissa]
    sums = [sum(row) for row in quadrature]
    c = {name: jnp.asarray(value) for name, value in constants().items()}
    node = lax.axis_index("node")
    place = (node * SLABS + lax.axis_index("space")).astype(jnp.int32).reshape(1)
    levels = (c["zlev0"], c["zlev1"], c["zlev2"])
    rows = (PLANES, 2, 128, NXY)
    tile = (2, 2, 2, 8, 128)
    modes = (4, 2, 2, 2, 8, 128)

    (sent,) = run(
        first_kernel,
        (initial, kappa, c["x_fwd"], c["y_first"]),
        [(2, 2, 4, 2, 2, 8, 128)],
        [
            (2, PLANES, 2, 16, NXY),
            (2, PLANES, 32, NXY),
            (PLANES, NXY, NXY),
            (PLANES, NXY, NXY),
            pltpu.VMEM((2, NXY, NXY), jnp.bfloat16),
            pltpu.VMEM((32, 3 * NXY), jnp.bfloat16),
            pltpu.SemaphoreType.DMA((10,)),
        ],
        scalar=place,
        far=True,
    )
    tables = (c["ytable"], c["xtable"])
    half = (4, 2, 8, 128)
    held = lax.all_to_all(sent.reshape(SLABS, 2, 8, 128), "space", 0, 0, tiled=True)
    sent, sections, start, *weights = run(
        functools.partial(start_kernel, shifts, sums),
        (held, c["z_fwd"], c["z_inv"], *levels, *tables),
        [(NODES, SLABS, 8, 128), (NODES,) + modes, modes]
        + [(NODES,) + modes] * 4
        + [(NODES,) + half] * 3,
        [modes, (NODES,) + modes, (NODES,) + modes, (NODES,) + half],
        scalar=place,
    )
    both = ("node", "space")
    count = NODES * SLABS
    held = lax.all_to_all(sent.reshape(count, 8, 128), both, 0, 0, tiled=True)
    (sent,) = run(
        middle_kernel,
        (held.reshape(16, 2, 4, 2, 8, 128), kappa, c["x_fwd"], c["x_inv"], c["y_fwd"], c["y_inv"]),
        [(16, 2, 4, 2, 8, 128)],
        [rows, (PLANES, NXY, NXY)],
    )
    held = lax.all_to_all(sent.reshape(count, 8, 128), both, 0, 0, tiled=True)
    (sent,) = run(
        functools.partial(step_kernel, shifts, quadrature),
        (held.reshape(NODES, SLABS, 8, 128), sections, start, c["z_fwd"], c["z_inv"], c["zlev0"], *weights, *tables),
        [(NODES, SLABS, 8, 128)],
        [(NODES,) + modes, (NODES,) + tile, (NODES,) + modes, (NODES,) + modes, (NODES,) + half],
        scalar=place,
    )
    held = lax.all_to_all(sent.reshape(count, 8, 128), both, 0, 0, tiled=True)
    (out,) = run(
        last_kernel,
        (held.reshape(16, 2, 4, 2, 8, 128), c["x_inv"], c["y_inv"]),
        [(1, PLANES, NXY, NXY)],
        [rows, (PLANES, NXY, NXY), pltpu.SemaphoreType.DMA((PLANES,))],
        far_out=True,
    )
    return out


def solution(mesh):
    in_specs = (P("space", None, None), P("space", None, None))
    out_specs = P("node", "space", None, None)
    return jax.shard_map(
        per_device, mesh=mesh, in_specs=in_specs, out_specs=out_specs, check_vma=False
    )
```

```python
import functools

import jax
import jax.numpy as jnp
import ml_dtypes
import numpy as np
from jax import lax
from jax.experimental import pallas as pl
from jax.experimental.pallas import tpu as pltpu
from jax.sharding import PartitionSpec as P

DIFFUSE = 2.0
REACT = 0.5
OMEGA = 0.8
NODES = 8
SLABS = 32
PLANES = 4
NZ = 128
NXY = 256
VCYCLES = 2


def radau_gap(count, where):
    previous = 1.0
    current = where
    for degree in range(1, count):
        following = ((2 * degree + 1) * where * current - degree * previous) / (degree + 1)
        previous = current
        current = following
    return current - previous


def radau_table(count):
    zeros_found = []
    grid_count = 4096
    lower = -1.0
    value_low = radau_gap(count, lower)
    for place in range(1, grid_count):
        upper = -1.0 + 2.0 * place / grid_count
        value_up = radau_gap(count, upper)
        if value_low * value_up < 0.0:
            left_end = lower
            right_end = upper
            left_value = value_low
            for halving in range(100):
                middle = 0.5 * (left_end + right_end)
                middle_value = radau_gap(count, middle)
                if left_value * middle_value <= 0.0:
                    right_end = middle
                else:
                    left_end = middle
                    left_value = middle_value
            zeros_found.append(0.5 * (left_end + right_end))
        lower = upper
        value_low = value_up
    zeros_found.append(1.0)
    abscissa = [(value + 1.0) / 2.0 for value in zeros_found]
    table_rows = []
    for outer in range(count):
        table_rows.append([0.0] * count)
    for column in range(count):
        factor = [1.0]
        scale = 1.0
        for other in range(count):
            if other != column:
                widened = [0.0] * (len(factor) + 1)
                for power in range(len(factor)):
                    widened[power + 1] = widened[power + 1] + factor[power]
                    widened[power] = widened[power] - abscissa[other] * factor[power]
                factor = widened
                scale = scale * (abscissa[column] - abscissa[other])
        for outer in range(count):
            upto = abscissa[outer]
            accum = 0.0
            for power in range(len(factor)):
                accum = accum + factor[power] * upto ** (power + 1) / (power + 1)
            table_rows[outer][column] = accum / scale
    return (abscissa, table_rows)


def mode_list(n):
    return [("c", k) for k in range(n // 2)] + [("s", k) for k in range(1, n // 2 + 1)]


def mode_vector(n, kind, k):
    angle = 2.0 * np.pi * k * (np.arange(n) + 0.5) / n
    values = np.cos(angle) if kind == "c" else np.sin(angle)
    return values / np.sqrt((values * values).sum())


def child_mode(coarse, kind, k, which):
    if which == 0:
        return (kind, k)
    if kind == "c":
        return ("s", coarse) if k == 0 else ("c", coarse - k)
    return ("c", coarse // 2) if k == coarse // 2 else ("s", coarse - k)


def pair_mean(n):
    return np.kron(np.eye(n // 2), np.full((1, 2), 0.5))


def dimension_tables(n):
    mid, low = n // 2, n // 4
    basis = np.zeros((2, 2, low, n))
    basis1 = np.zeros((2, low, mid))
    basis2 = np.zeros((low, low))
    ring0, ring1, ring2 = np.zeros((2, 2, low)), np.zeros((2, low)), np.zeros(low)
    for i, (kind, k) in enumerate(mode_list(low)):
        basis2[i] = mode_vector(low, kind, k)
        ring2[i] = 2.0 * np.cos(2.0 * np.pi * k / low)
        for b in range(2):
            kind1, k1 = child_mode(low, kind, k, b)
            basis1[b, i] = mode_vector(mid, kind1, k1)
            ring1[b, i] = 2.0 * np.cos(2.0 * np.pi * k1 / mid)
            for a in range(2):
                kind0, k0 = child_mode(mid, kind1, k1, a)
                basis[a, b, i] = mode_vector(n, kind0, k0)
                ring0[a, b, i] = 2.0 * np.cos(2.0 * np.pi * k0 / n)
    mean0 = np.einsum("bin,abin->abi", basis1 @ pair_mean(n), basis)
    mean1 = np.einsum("in,bin->bi", basis2 @ pair_mean(mid), basis1)
    return basis, ring0, mean0, ring1, mean1, ring2


def halves(matrix):
    high = matrix.astype(ml_dtypes.bfloat16)
    rest = (matrix - high.astype(np.float64)).astype(ml_dtypes.bfloat16)
    return np.stack([high, rest])


@functools.lru_cache(maxsize=None)
def constants():
    basis, ring0, mean0, ring1, mean1, ring2 = dimension_tables(NXY)
    low = NXY // 4
    to_x = basis.reshape(2, 2, 2, 2, 16, NXY).transpose(2, 0, 3, 1, 4, 5).reshape(NXY, NXY)
    to_y = basis.transpose(1, 2, 0, 3).reshape(NXY, NXY)
    first_y = basis.transpose(1, 2, 0, 3).reshape(2, NODES, 16, NXY)
    first_y = first_y.transpose(1, 0, 2, 3).reshape(NODES, 32, NXY)

    zbasis, zring0, zmean0, zring1, zmean1, zring2 = dimension_tables(NZ)
    along = zbasis.reshape(NZ, SLABS, PLANES)
    to_z = np.einsum("ac,kgisz->gakiszc", np.eye(2), along.reshape(4, 4, 8, SLABS, PLANES))
    to_z = to_z.reshape(2 * NZ, 2 * NZ)

    wide = lambda v: np.repeat(v[..., None], 128, axis=-1)
    grouped = lambda v: np.moveaxis(v.reshape(v.shape[:-1] + (4, 8)), -2, 0)
    zlev0 = wide(np.stack([grouped(zring0), grouped(zmean0)]))
    zlev1 = wide(np.stack([grouped(zring1), grouped(zmean1)]))
    zlev2 = wide(grouped(zring2))

    lanes = lambda v: np.broadcast_to(v, v.shape[:-4] + (2, 2, 2, 16)).reshape(v.shape[:-4] + (128,))
    ytable = np.zeros((low, 8, 128))
    for base in range(low):
        over_b = lambda v: lanes(v[:, base].reshape(1, 2, 1, 1))
        for a in range(2):
            ytable[base, a] = over_b(ring0[a])
            ytable[base, 2 + a] = over_b(mean0[a])
        ytable[base, 4] = over_b(ring1)
        ytable[base, 5] = over_b(mean1)
        ytable[base, 6] = ring2[base]
    xtable = np.zeros((4, 8, 128))
    for q in range(4):
        xs = slice(q * 16, q * 16 + 16)
        for a in range(2):
            xtable[q, a] = lanes(ring0[:, None, :, xs])
            xtable[q, 2 + a] = lanes(mean0[:, None, :, xs])
        xtable[q, 4] = lanes(ring1[None, None, :, xs])
        xtable[q, 5] = lanes(mean1[None, None, :, xs])
        xtable[q, 6] = lanes(ring2[None, None, None, xs])
    f32 = lambda v: np.asarray(v, np.float32)
    return {
        "x_fwd": halves(to_x.T.copy()),
        "x_inv": halves(to_x),
        "y_fwd": halves(to_y),
        "y_inv": halves(to_y.T.copy()),
        "y_first": np.concatenate([halves(first_y)[i] for i in (0, 0, 1)], axis=2),
        "z_fwd": halves(to_z),
        "z_inv": halves(to_z.T.copy()),
        "zlev0": f32(zlev0),
        "zlev1": f32(zlev1),
        "zlev2": f32(zlev2),
        "ytable": f32(ytable),
        "xtable": f32(xtable),
    }


def split(value):
    high = value.astype(jnp.bfloat16)
    return high, (value - high.astype(jnp.float32)).astype(jnp.bfloat16)


def product(a, b):
    return jnp.dot(a, b, preferred_element_type=jnp.float32)


def times(left, matrix):
    a, b = split(left)
    count = left.shape[0]
    both = product(jnp.concatenate([a, b], axis=0), matrix[0])
    return (both[:count] + both[count:]) + product(a, matrix[1])


def apply(matrix, right):
    a, b = split(right)
    count = matrix.shape[1]
    both = product(matrix[...].reshape(2 * count, matrix.shape[2]), a)
    return (both[:count] + both[count:]) + product(matrix[0], b)


def exchange(low, high, shift, keep):
    size = low.shape[0 if shift < 8 else 1]
    axis = 0 if shift < 8 else 1
    first = jnp.where(keep, low, pltpu.roll(high, shift, axis))
    second = jnp.where(keep, pltpu.roll(low, size - shift, axis), high)
    return first, second


def shuffle_lanes(pairs):
    keep = lax.broadcasted_iota(jnp.int32, (8, 128), 1) % 64 < 32
    return [exchange(a, b, 32, keep) for a, b in pairs]


def shuffle_rows(four):
    row = lax.broadcasted_iota(jnp.int32, (8, 128), 0)
    top, even = row < 4, row % 4 < 2
    a0, b0 = exchange(four[0], four[2], 4, top)
    a1, b1 = exchange(four[1], four[3], 4, top)
    c0, c1 = exchange(a0, a1, 2, even)
    c2, c3 = exchange(b0, b1, 2, even)
    return [c0, c1, c2, c3]


def pack(read, write):
    pairs = shuffle_lanes([(read(z, 0), read(z, 1)) for z in range(PLANES)])
    for qb in range(2):
        for inner, chunk in enumerate(shuffle_rows([pairs[z][qb] for z in range(PLANES)])):
            write(inner, qb, chunk)


def unpack(read, write):
    columns = [shuffle_rows([read(inner, qb) for inner in range(4)]) for qb in range(2)]
    for z in range(PLANES):
        ((first, second),) = shuffle_lanes([(columns[0][z], columns[1][z])])
        write(z, 0, first)
        write(z, 1, second)


def cubic(u, strength):
    return REACT * strength * (u - u * u * u)


def first_kernel(
    place, u_far, k_far, x_far, y_far, out_ref, rows, part, u_near, k_near, x_near, y_near, sems
):
    me = place[0] // SLABS
    copies = [pltpu.make_async_copy(y_far.at[me], y_near, sems.at[0])]
    for z in range(PLANES):
        copies.append(pltpu.make_async_copy(u_far.at[z], u_near.at[z], sems.at[2 * z + 1]))
        copies.append(pltpu.make_async_copy(k_far.at[z], k_near.at[z], sems.at[2 * z + 2]))
    copies.append(pltpu.make_async_copy(x_far, x_near, sems.at[9]))
    for copy in copies:
        copy.start()
    copies[0].wait()
    for z in range(PLANES):
        copies[2 * z + 1].wait()
        copies[2 * z + 2].wait()
        u = u_near[z]
        for array, field in enumerate((u, cubic(u, k_near[z]))):
            a, b = split(field)
            part[array, z] = product(y_near[...], jnp.concatenate([a, b, a], axis=0))
    copies[9].wait()
    for array in range(2):
        whole_part = times(part[array].reshape(PLANES * 32, NXY), x_near)
        rows[array] = whole_part.reshape(PLANES, 2, 16, NXY)
    for array in range(2):
        for g in range(2):
            for hq in range(2):
                lanes = slice(hq * 128, hq * 128 + 128)

                def read(z, b):
                    return rows[array, z, b, g * 8 : g * 8 + 8, lanes]

                def write(inner, qb, chunk):
                    out_ref[g, hq, inner, qb, array] = chunk

                pack(read, write)


def gather_rows(in_ref, rows):
    for kg in range(16):
        for hq in range(2):
            lanes = slice(hq * 128, hq * 128 + 128)

            def read(inner, qb):
                return in_ref[kg, hq, inner, qb]

            def write(z, b, tile):
                rows[z, b, kg * 8 : kg * 8 + 8, lanes] = tile

            unpack(read, write)


def scatter_rows(rows, out_ref):
    for kg in range(16):
        for hq in range(2):
            lanes = slice(hq * 128, hq * 128 + 128)

            def read(z, b):
                return rows[z, b, kg * 8 : kg * 8 + 8, lanes]

            def write(inner, qb, chunk):
                out_ref[kg, hq, inner, qb] = chunk

            pack(read, write)


def middle_kernel(in_ref, k_ref, x_fwd, x_inv, y_fwd, y_inv, out_ref, rows, part):
    gather_rows(in_ref, rows)
    for z in range(PLANES):
        part[z] = apply(y_inv, rows[z].reshape(NXY, NXY))
    for z in range(PLANES):
        part[z] = cubic(times(part[z], x_inv), k_ref[z])
    for z in range(PLANES):
        part[z] = times(part[z], x_fwd)
    for z in range(PLANES):
        rows[z] = apply(y_fwd, part[z]).reshape(2, 128, NXY)
    scatter_rows(rows, out_ref)


def last_kernel(in_ref, x_inv, y_inv, out_far, rows, part, sems):
    gather_rows(in_ref, rows)
    for z in range(PLANES):
        part[z] = apply(y_inv, rows[z].reshape(NXY, NXY))
    copies = []
    for z in range(PLANES):
        part[z] = times(part[z], x_inv)
        copies.append(pltpu.make_async_copy(part.at[z], out_far.at[0, z], sems.at[z]))
        copies[z].start()
    for copy in copies:
        copy.wait()


def lane_pair(value, distance):
    return value + pltpu.roll(value, distance, value.ndim - 1)


def mode_tables(group, zlev0, zlev1, zlev2, ytable, xtable):

    def row(i, join):
        return jnp.broadcast_to(join(ytable[0, i : i + 1], xtable[0, i : i + 1]), (8, 128))

    total = [row(i, jnp.add) for i in (0, 1, 4, 6)]
    scale = [row(i, jnp.multiply) for i in (2, 3, 5)]
    ring0 = [[[zlev0[0, group, c, d] + total[a] for d in range(2)] for c in range(2)] for a in range(2)]
    mean0 = [[[zlev0[1, group, c, d] * scale[a] for d in range(2)] for c in range(2)] for a in range(2)]
    ring1 = [zlev1[0, group, d] + total[2] for d in range(2)]
    mean1 = [zlev1[1, group, d] * scale[2] for d in range(2)]
    ring2 = zlev2[group] + total[3]
    three = lambda v: jnp.stack([jnp.stack([jnp.stack(y) for y in x]) for x in v])
    return three(ring0), three(mean0), jnp.stack(ring1), jnp.stack(mean1), ring2


def write_weights(shifts, tables, group, weights):
    quad, rise, lower, keep, down1, gain1, back1 = weights
    ring0, mean0, ring1, mean1, ring2 = tables
    for m, s in enumerate(shifts):
        s1, s2 = s / 4.0, s / 16.0
        weight = OMEGA / (1.0 + 6.0 * s)
        weight1, weight2 = OMEGA / (1.0 + 6.0 * s1), OMEGA / (1.0 + 6.0 * s2)
        sigma = (1.0 - OMEGA) + (weight * s) * ring0
        square = sigma * sigma
        scaled = mean0 * square
        quad[m, group] = square * square
        rise[m, group] = (square + 1.0) * (sigma + 1.0)
        lower[m, group] = scaled
        keep[m, group] = scaled * (sigma - 1.0)
        sigma1 = (1.0 - OMEGA) + (weight1 * s1) * ring1
        sigma2 = (1.0 - OMEGA) + (weight2 * s2) * ring2
        square1 = sigma1 * sigma1
        square2 = sigma2 * sigma2
        sweeps = (1.0 + sigma2) * (1.0 + square2) * ((64.0 * weight2 / weight1) * (1.0 + square2 * square2))
        passed = mean1 * square1
        down1[m, group] = (weight1 / weight) * passed
        gain1[m, group] = (8.0 * weight1 / weight) * ((1.0 + sigma1) * (1.0 + square1))
        back1[m, group] = passed * sweeps


def pair_sums(m, group, v, weights, down, sums):
    keep = weights[3]
    remain = keep[m, group] * v + down
    sums[m, group] = (remain[0, 0] + remain[0, 1]) + (remain[1, 0] + remain[1, 1])


def correction(m, weights, sums):
    down1, gain1, back1 = weights[4:]
    source1 = lane_pair(sums[m], 64)
    lower = down1[m] * source1
    total = lower[:, 0] + lower[:, 1]
    turns = [pltpu.roll(total, 16 * k, 2) for k in range(1, 4)]
    total = (total + turns[0]) + (turns[1] + turns[2])
    sums[m] = gain1[m] * source1 + back1[m] * total[:, None]


def finish_cycles(weights, first, v, base, down, sums, z_inv, out_ref):
    quad, lower = weights[0], weights[2]
    for cycle in range(VCYCLES):
        before = first if cycle == 0 else v
        for m in range(NODES):
            correction(m, weights, sums)
            for group in range(4):
                field = quad[m, group] * before[m, group] + base[m, group]
                field = field + lower[m, group] * sums[m, group]
                v[m, group] = field
                if cycle + 1 < VCYCLES:
                    pair_sums(m, group, field, weights, down[m, group], sums)
            if cycle + 1 == VCYCLES and m % 2 == 1:
                to_slabs(m // 2, v, z_inv, out_ref)


def place_rows(place, ytable, xtable):
    base = place // 16 * 4 + place // 2 % 4
    part = place // 8 % 2 * 2 + place % 2
    return ytable.at[pl.ds(base, 1)], xtable.at[pl.ds(part, 1)]


def laplacian(zlev0, group, ytable, xtable):
    near = [
        jnp.broadcast_to(ytable[0, a : a + 1] + xtable[0, a : a + 1] - 6.0, (8, 128))
        for a in range(2)
    ]
    line = zlev0[0, group]
    return jnp.stack([line + near[a] for a in range(2)])


def to_slabs(pair, modes, z_inv, out_ref):
    both = jnp.concatenate([modes[2 * pair + i].reshape(2 * NZ, 128) for i in range(2)], axis=1)
    both = apply(z_inv, both)
    for i in range(2):
        out_ref[2 * pair + i] = both[:, i * 128 : i * 128 + 128].reshape(SLABS, 8, 128)


def start_kernel(
    shifts, sums, place, in_ref, z_fwd, z_inv, zlev0, zlev1, zlev2, ytable, xtable,
    out_ref, sections, start, quad, rise, lower, keep, down1, gain1, back1,
    cubes, base, down, pairs,
):
    weights = (quad, rise, lower, keep, down1, gain1, back1)
    ytable, xtable = place_rows(place[0], ytable, xtable)
    both = jnp.concatenate([in_ref[:, i].reshape(2 * NZ, 128) for i in range(2)], axis=1)
    both = apply(z_fwd, both)
    start[...] = both[:, :128].reshape(4, 2, 2, 2, 8, 128)
    cubes[...] = both[:, 128:].reshape(4, 2, 2, 2, 8, 128)

    def group_step(group, carry):
        tables = mode_tables(group, zlev0, zlev1, zlev2, ytable, xtable)
        write_weights(shifts, tables, group, weights)
        lap = tables[0] - 6.0
        u = start[group]
        cube = cubes[group]
        for m, s in enumerate(shifts):
            weight = OMEGA / (1.0 + 6.0 * s)
            source = (weight + (weight * (DIFFUSE * sums[m] - s)) * lap) * u + (weight * sums[m]) * cube
            base[m, group] = rise[m, group] * source
            passed = lower[m, group] * source
            down[m, group] = passed
            sections[m, group] = u
            pair_sums(m, group, u, weights, passed, pairs)
        return carry

    lax.fori_loop(0, 4, group_step, 0, unroll=True)
    finish_cycles(weights, sections, sections, base, down, pairs, z_inv, out_ref)


def step_kernel(
    shifts, quadrature, place, in_ref, sections, start, z_fwd, z_inv, zlev0, quad, rise, lower, keep,
    down1, gain1, back1, ytable, xtable, out_ref, cubes, force, base, down, pairs,
):
    weights = (quad, rise, lower, keep, down1, gain1, back1)
    ytable, xtable = place_rows(place[0], ytable, xtable)
    for pair in range(NODES // 2):
        both = jnp.concatenate(
            [in_ref[2 * pair + i].reshape(2 * NZ, 128) for i in range(2)], axis=1
        )
        both = apply(z_fwd, both)
        for i in range(2):
            part = both[:, i * 128 : i * 128 + 128]
            cubes[2 * pair + i] = part.reshape(4, 2, 2, 2, 8, 128)

    def group_step(group, carry):
        lap = laplacian(zlev0, group, ytable, xtable)
        double = DIFFUSE * lap
        for m in range(NODES):
            force[m] = double * sections[m, group] + cubes[m, group]
        for m, s in enumerate(shifts):
            u = sections[m, group]
            weight = OMEGA / (1.0 + 6.0 * s)
            source = weight * start[group] - (weight * s) * (lap * u)
            for j in range(NODES):
                source = source + (weight * quadrature[m][j]) * force[j]
            base[m, group] = rise[m, group] * source
            passed = lower[m, group] * source
            down[m, group] = passed
            pair_sums(m, group, u, weights, passed, pairs)
        return carry

    lax.fori_loop(0, 4, group_step, 0, unroll=True)
    finish_cycles(weights, sections, cubes, base, down, pairs, z_inv, out_ref)


def whole(shape):
    return pl.BlockSpec(shape, lambda *_: (0,) * len(shape))


FAR = pl.BlockSpec(memory_space=pltpu.MemorySpace.HBM)


def run(kernel, args, outs, scratch, scalar=None, far=False, far_out=False):
    specs = [FAR if far else whole(a.shape) for a in args]
    out_shape = [jax.ShapeDtypeStruct(shape, jnp.float32) for shape in outs]
    out_specs = [FAR if far_out else whole(shape) for shape in outs]
    grid_spec = pltpu.PrefetchScalarGridSpec(
        num_scalar_prefetch=0 if scalar is None else 1,
        grid=(1,),
        in_specs=specs,
        out_specs=out_specs,
        scratch_shapes=[pltpu.VMEM(s, jnp.float32) if isinstance(s, tuple) else s for s in scratch],
    )
    call = pl.pallas_call(
        kernel,
        grid_spec=grid_spec,
        out_shape=out_shape,
        compiler_params=pltpu.CompilerParams(vmem_limit_bytes=40 * 1024 * 1024),
    )
    if far:
        args = [pltpu.with_memory_space_constraint(a, pltpu.MemorySpace.HBM) for a in args]
    return call(*([] if scalar is None else [scalar]), *args)


def per_device(initial, kappa):
    abscissa, quadrature = radau_table(NODES)
    shifts = [DIFFUSE * value for value in abscissa]
    sums = [sum(row) for row in quadrature]
    c = {name: jnp.asarray(value) for name, value in constants().items()}
    node = lax.axis_index("node")
    place = (node * SLABS + lax.axis_index("space")).astype(jnp.int32).reshape(1)
    levels = (c["zlev0"], c["zlev1"], c["zlev2"])
    rows = (PLANES, 2, 128, NXY)
    tile = (2, 2, 2, 8, 128)
    modes = (4, 2, 2, 2, 8, 128)

    (sent,) = run(
        first_kernel,
        (initial, kappa, c["x_fwd"], c["y_first"]),
        [(2, 2, 4, 2, 2, 8, 128)],
        [
            (2, PLANES, 2, 16, NXY),
            (2, PLANES, 32, NXY),
            (PLANES, NXY, NXY),
            (PLANES, NXY, NXY),
            pltpu.VMEM((2, NXY, NXY), jnp.bfloat16),
            pltpu.VMEM((32, 3 * NXY), jnp.bfloat16),
            pltpu.SemaphoreType.DMA((10,)),
        ],
        scalar=place,
        far=True,
    )
    tables = (c["ytable"], c["xtable"])
    half = (4, 2, 8, 128)
    held = lax.all_to_all(sent.reshape(SLABS, 2, 8, 128), "space", 0, 0, tiled=True)
    sent, sections, start, *weights = run(
        functools.partial(start_kernel, shifts, sums),
        (held, c["z_fwd"], c["z_inv"], *levels, *tables),
        [(NODES, SLABS, 8, 128), (NODES,) + modes, modes]
        + [(NODES,) + modes] * 4
        + [(NODES,) + half] * 3,
        [modes, (NODES,) + modes, (NODES,) + modes, (NODES,) + half],
        scalar=place,
    )
    both = ("node", "space")
    count = NODES * SLABS
    held = lax.all_to_all(sent.reshape(count, 8, 128), both, 0, 0, tiled=True)
    (sent,) = run(
        middle_kernel,
        (held.reshape(16, 2, 4, 2, 8, 128), kappa, c["x_fwd"], c["x_inv"], c["y_fwd"], c["y_inv"]),
        [(16, 2, 4, 2, 8, 128)],
        [rows, (PLANES, NXY, NXY)],
    )
    held = lax.all_to_all(sent.reshape(count, 8, 128), both, 0, 0, tiled=True)
    (sent,) = run(
        functools.partial(step_kernel, shifts, quadrature),
        (held.reshape(NODES, SLABS, 8, 128), sections, start, c["z_fwd"], c["z_inv"], c["zlev0"], *weights, *tables),
        [(NODES, SLABS, 8, 128)],
        [(NODES,) + modes, (NODES,) + tile, (NODES,) + modes, (NODES,) + modes, (NODES,) + half],
        scalar=place,
    )
    held = lax.all_to_all(sent.reshape(count, 8, 128), both, 0, 0, tiled=True)
    (out,) = run(
        last_kernel,
        (held.reshape(16, 2, 4, 2, 8, 128), c["x_inv"], c["y_inv"]),
        [(1, PLANES, NXY, NXY)],
        [rows, (PLANES, NXY, NXY), pltpu.SemaphoreType.DMA((PLANES,))],
        far_out=True,
    )
    return out


def solution(mesh):
    in_specs = (P("space", None, None), P("space", None, None))
    out_specs = P("node", "space", None, None)
    return jax.shard_map(
        per_device, mesh=mesh, in_specs=in_specs, out_specs=out_specs, check_vma=False
    )
```

```python
import functools

import jax
import jax.numpy as jnp
import ml_dtypes
import numpy as np
from jax import lax
from jax.experimental import pallas as pl
from jax.experimental.pallas import tpu as pltpu
from jax.sharding import PartitionSpec as P

DIFFUSE = 2.0
REACT = 0.5
OMEGA = 0.8
NODES = 8
SLABS = 32
PLANES = 4
NZ = 128
NXY = 256
VCYCLES = 2


def radau_gap(count, where):
    previous = 1.0
    current = where
    for degree in range(1, count):
        following = ((2 * degree + 1) * where * current - degree * previous) / (degree + 1)
        previous = current
        current = following
    return current - previous


def radau_table(count):
    zeros_found = []
    grid_count = 4096
    lower = -1.0
    value_low = radau_gap(count, lower)
    for place in range(1, grid_count):
        upper = -1.0 + 2.0 * place / grid_count
        value_up = radau_gap(count, upper)
        if value_low * value_up < 0.0:
            left_end = lower
            right_end = upper
            left_value = value_low
            for halving in range(100):
                middle = 0.5 * (left_end + right_end)
                middle_value = radau_gap(count, middle)
                if left_value * middle_value <= 0.0:
                    right_end = middle
                else:
                    left_end = middle
                    left_value = middle_value
            zeros_found.append(0.5 * (left_end + right_end))
        lower = upper
        value_low = value_up
    zeros_found.append(1.0)
    abscissa = [(value + 1.0) / 2.0 for value in zeros_found]
    table_rows = []
    for outer in range(count):
        table_rows.append([0.0] * count)
    for column in range(count):
        factor = [1.0]
        scale = 1.0
        for other in range(count):
            if other != column:
                widened = [0.0] * (len(factor) + 1)
                for power in range(len(factor)):
                    widened[power + 1] = widened[power + 1] + factor[power]
                    widened[power] = widened[power] - abscissa[other] * factor[power]
                factor = widened
                scale = scale * (abscissa[column] - abscissa[other])
        for outer in range(count):
            upto = abscissa[outer]
            accum = 0.0
            for power in range(len(factor)):
                accum = accum + factor[power] * upto ** (power + 1) / (power + 1)
            table_rows[outer][column] = accum / scale
    return (abscissa, table_rows)


def mode_list(n):
    return [("c", k) for k in range(n // 2)] + [("s", k) for k in range(1, n // 2 + 1)]


def mode_vector(n, kind, k):
    angle = 2.0 * np.pi * k * (np.arange(n) + 0.5) / n
    values = np.cos(angle) if kind == "c" else np.sin(angle)
    return values / np.sqrt((values * values).sum())


def child_mode(coarse, kind, k, which):
    if which == 0:
        return (kind, k)
    if kind == "c":
        return ("s", coarse) if k == 0 else ("c", coarse - k)
    return ("c", coarse // 2) if k == coarse // 2 else ("s", coarse - k)


def pair_mean(n):
    return np.kron(np.eye(n // 2), np.full((1, 2), 0.5))


def dimension_tables(n):
    mid, low = n // 2, n // 4
    basis = np.zeros((2, 2, low, n))
    basis1 = np.zeros((2, low, mid))
    basis2 = np.zeros((low, low))
    ring0, ring1, ring2 = np.zeros((2, 2, low)), np.zeros((2, low)), np.zeros(low)
    for i, (kind, k) in enumerate(mode_list(low)):
        basis2[i] = mode_vector(low, kind, k)
        ring2[i] = 2.0 * np.cos(2.0 * np.pi * k / low)
        for b in range(2):
            kind1, k1 = child_mode(low, kind, k, b)
            basis1[b, i] = mode_vector(mid, kind1, k1)
            ring1[b, i] = 2.0 * np.cos(2.0 * np.pi * k1 / mid)
            for a in range(2):
                kind0, k0 = child_mode(mid, kind1, k1, a)
                basis[a, b, i] = mode_vector(n, kind0, k0)
                ring0[a, b, i] = 2.0 * np.cos(2.0 * np.pi * k0 / n)
    mean0 = np.einsum("bin,abin->abi", basis1 @ pair_mean(n), basis)
    mean1 = np.einsum("in,bin->bi", basis2 @ pair_mean(mid), basis1)
    return basis, ring0, mean0, ring1, mean1, ring2


def halves(matrix):
    high = matrix.astype(ml_dtypes.bfloat16)
    rest = (matrix - high.astype(np.float64)).astype(ml_dtypes.bfloat16)
    return np.stack([high, rest])


@functools.lru_cache(maxsize=None)
def constants():
    basis, ring0, mean0, ring1, mean1, ring2 = dimension_tables(NXY)
    low = NXY // 4
    to_x = basis.reshape(2, 2, 2, 2, 16, NXY).transpose(2, 0, 3, 1, 4, 5).reshape(NXY, NXY)
    to_y = basis.transpose(1, 2, 0, 3).reshape(NXY, NXY)
    first_y = basis.transpose(1, 2, 0, 3).reshape(2, NODES, 16, NXY)
    first_y = first_y.transpose(1, 0, 2, 3).reshape(NODES, 32, NXY)

    zbasis, zring0, zmean0, zring1, zmean1, zring2 = dimension_tables(NZ)
    along = zbasis.reshape(NZ, SLABS, PLANES)
    to_z = np.einsum("ac,kgisz->gakiszc", np.eye(2), along.reshape(4, 4, 8, SLABS, PLANES))
    to_z = to_z.reshape(2 * NZ, 2 * NZ)

    wide = lambda v: np.repeat(v[..., None], 128, axis=-1)
    grouped = lambda v: np.moveaxis(v.reshape(v.shape[:-1] + (4, 8)), -2, 0)
    zlev0 = wide(np.stack([grouped(zring0), grouped(zmean0)]))
    zlev1 = wide(np.stack([grouped(zring1), grouped(zmean1)]))
    zlev2 = wide(grouped(zring2))

    lanes = lambda v: np.broadcast_to(v, v.shape[:-4] + (2, 2, 2, 16)).reshape(v.shape[:-4] + (128,))
    ytable = np.zeros((low, 8, 128))
    for base in range(low):
        over_b = lambda v: lanes(v[:, base].reshape(1, 2, 1, 1))
        for a in range(2):
            ytable[base, a] = over_b(ring0[a])
            ytable[base, 2 + a] = over_b(mean0[a])
        ytable[base, 4] = over_b(ring1)
        ytable[base, 5] = over_b(mean1)
        ytable[base, 6] = ring2[base]
    xtable = np.zeros((4, 8, 128))
    for q in range(4):
        xs = slice(q * 16, q * 16 + 16)
        for a in range(2):
            xtable[q, a] = lanes(ring0[:, None, :, xs])
            xtable[q, 2 + a] = lanes(mean0[:, None, :, xs])
        xtable[q, 4] = lanes(ring1[None, None, :, xs])
        xtable[q, 5] = lanes(mean1[None, None, :, xs])
        xtable[q, 6] = lanes(ring2[None, None, None, xs])
    f32 = lambda v: np.asarray(v, np.float32)
    return {
        "x_fwd": halves(to_x.T.copy()),
        "x_inv": halves(to_x),
        "y_fwd": halves(to_y),
        "y_inv": halves(to_y.T.copy()),
        "y_first": np.concatenate([halves(first_y)[i] for i in (0, 0, 1)], axis=2),
        "z_fwd": halves(to_z),
        "z_inv": halves(to_z.T.copy()),
        "zlev0": f32(zlev0),
        "zlev1": f32(zlev1),
        "zlev2": f32(zlev2),
        "ytable": f32(ytable),
        "xtable": f32(xtable),
    }


def split(value):
    high = value.astype(jnp.bfloat16)
    return high, (value - high.astype(jnp.float32)).astype(jnp.bfloat16)


def product(a, b):
    return jnp.dot(a, b, preferred_element_type=jnp.float32)


def times(left, matrix):
    a, b = split(left)
    count = left.shape[0]
    both = product(jnp.concatenate([a, b], axis=0), matrix[0])
    return (both[:count] + both[count:]) + product(a, matrix[1])


def apply(matrix, right):
    a, b = split(right)
    count = matrix.shape[1]
    both = product(matrix[...].reshape(2 * count, matrix.shape[2]), a)
    return (both[:count] + both[count:]) + product(matrix[0], b)


def exchange(low, high, shift, keep):
    size = low.shape[0 if shift < 8 else 1]
    axis = 0 if shift < 8 else 1
    first = jnp.where(keep, low, pltpu.roll(high, shift, axis))
    second = jnp.where(keep, pltpu.roll(low, size - shift, axis), high)
    return first, second


def shuffle_lanes(pairs):
    keep = lax.broadcasted_iota(jnp.int32, (8, 128), 1) % 64 < 32
    return [exchange(a, b, 32, keep) for a, b in pairs]


def shuffle_rows(four):
    row = lax.broadcasted_iota(jnp.int32, (8, 128), 0)
    top, even = row < 4, row % 4 < 2
    a0, b0 = exchange(four[0], four[2], 4, top)
    a1, b1 = exchange(four[1], four[3], 4, top)
    c0, c1 = exchange(a0, a1, 2, even)
    c2, c3 = exchange(b0, b1, 2, even)
    return [c0, c1, c2, c3]


def pack(read, write):
    pairs = shuffle_lanes([(read(z, 0), read(z, 1)) for z in range(PLANES)])
    for qb in range(2):
        for inner, chunk in enumerate(shuffle_rows([pairs[z][qb] for z in range(PLANES)])):
            write(inner, qb, chunk)


def unpack(read, write):
    columns = [shuffle_rows([read(inner, qb) for inner in range(4)]) for qb in range(2)]
    for z in range(PLANES):
        ((first, second),) = shuffle_lanes([(columns[0][z], columns[1][z])])
        write(z, 0, first)
        write(z, 1, second)


def cubic(u, strength):
    return REACT * strength * (u - u * u * u)


def first_kernel(
    place, u_far, k_far, x_far, y_far, out_ref, rows, part, u_near, k_near, x_near, y_near, sems
):
    me = place[0] // SLABS
    copies = [pltpu.make_async_copy(y_far.at[me], y_near, sems.at[0])]
    for z in range(PLANES):
        copies.append(pltpu.make_async_copy(u_far.at[z], u_near.at[z], sems.at[2 * z + 1]))
        copies.append(pltpu.make_async_copy(k_far.at[z], k_near.at[z], sems.at[2 * z + 2]))
    copies.append(pltpu.make_async_copy(x_far, x_near, sems.at[9]))
    for copy in copies:
        copy.start()
    copies[0].wait()
    for z in range(PLANES):
        copies[2 * z + 1].wait()
        copies[2 * z + 2].wait()
        u = u_near[z]
        for array, field in enumerate((u, cubic(u, k_near[z]))):
            a, b = split(field)
            part[array, z] = product(y_near[...], jnp.concatenate([a, b, a], axis=0))
    copies[9].wait()
    for array in range(2):
        whole_part = times(part[array].reshape(PLANES * 32, NXY), x_near)
        rows[array] = whole_part.reshape(PLANES, 2, 16, NXY)
    for array in range(2):
        for g in range(2):
            for hq in range(2):
                lanes = slice(hq * 128, hq * 128 + 128)

                def read(z, b):
                    return rows[array, z, b, g * 8 : g * 8 + 8, lanes]

                def write(inner, qb, chunk):
                    out_ref[g, hq, inner, qb, array] = chunk

                pack(read, write)


def gather_rows(in_ref, rows):
    for kg in range(16):
        for hq in range(2):
            lanes = slice(hq * 128, hq * 128 + 128)

            def read(inner, qb):
                return in_ref[kg, hq, inner, qb]

            def write(z, b, tile):
                rows[z, b, kg * 8 : kg * 8 + 8, lanes] = tile

            unpack(read, write)


def scatter_rows(rows, out_ref):
    for kg in range(16):
        for hq in range(2):
            lanes = slice(hq * 128, hq * 128 + 128)

            def read(z, b):
                return rows[z, b, kg * 8 : kg * 8 + 8, lanes]

            def write(inner, qb, chunk):
                out_ref[kg, hq, inner, qb] = chunk

            pack(read, write)


def middle_kernel(in_ref, k_ref, x_fwd, x_inv, y_fwd, y_inv, out_ref, rows, part):
    gather_rows(in_ref, rows)
    for z in range(PLANES):
        part[z] = apply(y_inv, rows[z].reshape(NXY, NXY))
    for z in range(PLANES):
        part[z] = cubic(times(part[z], x_inv), k_ref[z])
    for z in range(PLANES):
        part[z] = times(part[z], x_fwd)
    for z in range(PLANES):
        rows[z] = apply(y_fwd, part[z]).reshape(2, 128, NXY)
    scatter_rows(rows, out_ref)


def last_kernel(in_ref, x_inv, y_inv, out_far, rows, part, sems):
    gather_rows(in_ref, rows)
    for z in range(PLANES):
        part[z] = apply(y_inv, rows[z].reshape(NXY, NXY))
    copies = []
    for z in range(PLANES):
        part[z] = times(part[z], x_inv)
        copies.append(pltpu.make_async_copy(part.at[z], out_far.at[0, z], sems.at[z]))
        copies[z].start()
    for copy in copies:
        copy.wait()


def lane_pair(value, distance):
    return value + pltpu.roll(value, distance, value.ndim - 1)


def mode_tables(group, zlev0, zlev1, zlev2, ytable, xtable):

    def row(i, join):
        return jnp.broadcast_to(join(ytable[0, i : i + 1], xtable[0, i : i + 1]), (8, 128))

    total = [row(i, jnp.add) for i in (0, 1, 4, 6)]
    scale = [row(i, jnp.multiply) for i in (2, 3, 5)]
    ring0 = [[[zlev0[0, group, c, d] + total[a] for d in range(2)] for c in range(2)] for a in range(2)]
    mean0 = [[[zlev0[1, group, c, d] * scale[a] for d in range(2)] for c in range(2)] for a in range(2)]
    ring1 = [zlev1[0, group, d] + total[2] for d in range(2)]
    mean1 = [zlev1[1, group, d] * scale[2] for d in range(2)]
    ring2 = zlev2[group] + total[3]
    three = lambda v: jnp.stack([jnp.stack([jnp.stack(y) for y in x]) for x in v])
    return three(ring0), three(mean0), jnp.stack(ring1), jnp.stack(mean1), ring2


def write_weights(shifts, tables, group, weights):
    quad, rise, lower, keep, down1, gain1, back1 = weights
    ring0, mean0, ring1, mean1, ring2 = tables
    for m, s in enumerate(shifts):
        s1, s2 = s / 4.0, s / 16.0
        weight = OMEGA / (1.0 + 6.0 * s)
        weight1, weight2 = OMEGA / (1.0 + 6.0 * s1), OMEGA / (1.0 + 6.0 * s2)
        sigma = (1.0 - OMEGA) + (weight * s) * ring0
        square = sigma * sigma
        scaled = mean0 * square
        quad[m, group] = square * square
        rise[m, group] = (square + 1.0) * (sigma + 1.0)
        lower[m, group] = scaled
        keep[m, group] = scaled * (sigma - 1.0)
        sigma1 = (1.0 - OMEGA) + (weight1 * s1) * ring1
        sigma2 = (1.0 - OMEGA) + (weight2 * s2) * ring2
        square1 = sigma1 * sigma1
        square2 = sigma2 * sigma2
        sweeps = (1.0 + sigma2) * (1.0 + square2) * ((64.0 * weight2 / weight1) * (1.0 + square2 * square2))
        passed = mean1 * square1
        down1[m, group] = (weight1 / weight) * passed
        gain1[m, group] = (8.0 * weight1 / weight) * ((1.0 + sigma1) * (1.0 + square1))
        back1[m, group] = passed * sweeps


def pair_sums(m, group, v, weights, down, sums):
    keep = weights[3]
    remain = keep[m, group] * v + down
    sums[m, group] = (remain[0, 0] + remain[0, 1]) + (remain[1, 0] + remain[1, 1])


def correction(m, weights, sums):
    down1, gain1, back1 = weights[4:]
    source1 = lane_pair(sums[m], 64)
    lower = down1[m] * source1
    total = lower[:, 0] + lower[:, 1]
    turns = [pltpu.roll(total, 16 * k, 2) for k in range(1, 4)]
    total = (total + turns[0]) + (turns[1] + turns[2])
    sums[m] = gain1[m] * source1 + back1[m] * total[:, None]


def finish_cycles(weights, first, v, base, down, sums, z_inv, out_ref):
    quad, lower = weights[0], weights[2]
    for cycle in range(VCYCLES):
        for m in range(NODES):
            correction(m, weights, sums)
            for group in range(4):
                before = first(m, group) if cycle == 0 else v[m, group]
                field = quad[m, group] * before + base[m, group]
                field = field + lower[m, group] * sums[m, group]
                v[m, group] = field
                if cycle + 1 < VCYCLES:
                    pair_sums(m, group, field, weights, down[m, group], sums)
            if cycle + 1 == VCYCLES and m % 2 == 1:
                to_slabs(m // 2, v, z_inv, out_ref)


def place_rows(place, ytable, xtable):
    base = place // 16 * 4 + place // 2 % 4
    part = place // 8 % 2 * 2 + place % 2
    return ytable.at[pl.ds(base, 1)], xtable.at[pl.ds(part, 1)]


def laplacian(zlev0, group, ytable, xtable):
    near = [
        jnp.broadcast_to(ytable[0, a : a + 1] + xtable[0, a : a + 1] - 6.0, (8, 128))
        for a in range(2)
    ]
    line = zlev0[0, group]
    return jnp.stack([line + near[a] for a in range(2)])


def to_slabs(pair, modes, z_inv, out_ref):
    both = jnp.concatenate([modes[2 * pair + i].reshape(2 * NZ, 128) for i in range(2)], axis=1)
    both = apply(z_inv, both)
    for i in range(2):
        out_ref[2 * pair + i] = both[:, i * 128 : i * 128 + 128].reshape(SLABS, 8, 128)


def start_kernel(
    shifts, sums, place, in_ref, z_fwd, z_inv, zlev0, zlev1, zlev2, ytable, xtable,
    out_ref, sections, start, quad, rise, lower, keep, down1, gain1, back1,
    cubes, base, down, pairs,
):
    weights = (quad, rise, lower, keep, down1, gain1, back1)
    ytable, xtable = place_rows(place[0], ytable, xtable)
    both = jnp.concatenate([in_ref[:, i].reshape(2 * NZ, 128) for i in range(2)], axis=1)
    both = apply(z_fwd, both)
    start[...] = both[:, :128].reshape(4, 2, 2, 2, 8, 128)
    cubes[...] = both[:, 128:].reshape(4, 2, 2, 2, 8, 128)

    def group_step(group, carry):
        tables = mode_tables(group, zlev0, zlev1, zlev2, ytable, xtable)
        write_weights(shifts, tables, group, weights)
        lap = tables[0] - 6.0
        u = start[group]
        cube = cubes[group]
        for m, s in enumerate(shifts):
            weight = OMEGA / (1.0 + 6.0 * s)
            source = (weight + (weight * (DIFFUSE * sums[m] - s)) * lap) * u + (weight * sums[m]) * cube
            base[m, group] = rise[m, group] * source
            passed = lower[m, group] * source
            down[m, group] = passed
            pair_sums(m, group, u, weights, passed, pairs)
        return carry

    lax.fori_loop(0, 4, group_step, 0, unroll=True)
    first = lambda m, group: start[group]
    finish_cycles(weights, first, sections, base, down, pairs, z_inv, out_ref)


def step_kernel(
    shifts, quadrature, place, in_ref, sections, start, z_fwd, z_inv, zlev0, quad, rise, lower, keep,
    down1, gain1, back1, ytable, xtable, out_ref, cubes, force, base, down, pairs,
):
    weights = (quad, rise, lower, keep, down1, gain1, back1)
    ytable, xtable = place_rows(place[0], ytable, xtable)
    for pair in range(NODES // 2):
        both = jnp.concatenate(
            [in_ref[2 * pair + i].reshape(2 * NZ, 128) for i in range(2)], axis=1
        )
        both = apply(z_fwd, both)
        for i in range(2):
            part = both[:, i * 128 : i * 128 + 128]
            cubes[2 * pair + i] = part.reshape(4, 2, 2, 2, 8, 128)

    def group_step(group, carry):
        lap = laplacian(zlev0, group, ytable, xtable)
        falls = []
        for m in range(NODES):
            falls.append(lap * sections[m, group])
            force[m] = DIFFUSE * falls[m] + cubes[m, group]
        for m, s in enumerate(shifts):
            u = sections[m, group]
            weight = OMEGA / (1.0 + 6.0 * s)
            source = weight * start[group] - (weight * s) * falls[m]
            for j in range(NODES):
                source = source + (weight * quadrature[m][j]) * force[j]
            base[m, group] = rise[m, group] * source
            passed = lower[m, group] * source
            down[m, group] = passed
            pair_sums(m, group, u, weights, passed, pairs)
        return carry

    lax.fori_loop(0, 4, group_step, 0, unroll=True)
    first = lambda m, group: sections[m, group]
    finish_cycles(weights, first, cubes, base, down, pairs, z_inv, out_ref)


def whole(shape):
    return pl.BlockSpec(shape, lambda *_: (0,) * len(shape))


FAR = pl.BlockSpec(memory_space=pltpu.MemorySpace.HBM)


def run(kernel, args, outs, scratch, scalar=None, far=False, far_out=False):
    specs = [FAR if far else whole(a.shape) for a in args]
    out_shape = [jax.ShapeDtypeStruct(shape, jnp.float32) for shape in outs]
    out_specs = [FAR if far_out else whole(shape) for shape in outs]
    grid_spec = pltpu.PrefetchScalarGridSpec(
        num_scalar_prefetch=0 if scalar is None else 1,
        grid=(1,),
        in_specs=specs,
        out_specs=out_specs,
        scratch_shapes=[pltpu.VMEM(s, jnp.float32) if isinstance(s, tuple) else s for s in scratch],
    )
    call = pl.pallas_call(
        kernel,
        grid_spec=grid_spec,
        out_shape=out_shape,
        compiler_params=pltpu.CompilerParams(vmem_limit_bytes=40 * 1024 * 1024),
    )
    if far:
        args = [pltpu.with_memory_space_constraint(a, pltpu.MemorySpace.HBM) for a in args]
    return call(*([] if scalar is None else [scalar]), *args)


def per_device(initial, kappa):
    abscissa, quadrature = radau_table(NODES)
    shifts = [DIFFUSE * value for value in abscissa]
    sums = [sum(row) for row in quadrature]
    c = {name: jnp.asarray(value) for name, value in constants().items()}
    node = lax.axis_index("node")
    place = (node * SLABS + lax.axis_index("space")).astype(jnp.int32).reshape(1)
    levels = (c["zlev0"], c["zlev1"], c["zlev2"])
    rows = (PLANES, 2, 128, NXY)
    tile = (2, 2, 2, 8, 128)
    modes = (4, 2, 2, 2, 8, 128)

    (sent,) = run(
        first_kernel,
        (initial, kappa, c["x_fwd"], c["y_first"]),
        [(2, 2, 4, 2, 2, 8, 128)],
        [
            (2, PLANES, 2, 16, NXY),
            (2, PLANES, 32, NXY),
            (PLANES, NXY, NXY),
            (PLANES, NXY, NXY),
            pltpu.VMEM((2, NXY, NXY), jnp.bfloat16),
            pltpu.VMEM((32, 3 * NXY), jnp.bfloat16),
            pltpu.SemaphoreType.DMA((10,)),
        ],
        scalar=place,
        far=True,
    )
    tables = (c["ytable"], c["xtable"])
    half = (4, 2, 8, 128)
    held = lax.all_to_all(sent.reshape(SLABS, 2, 8, 128), "space", 0, 0, tiled=True)
    sent, sections, start, *weights = run(
        functools.partial(start_kernel, shifts, sums),
        (held, c["z_fwd"], c["z_inv"], *levels, *tables),
        [(NODES, SLABS, 8, 128), (NODES,) + modes, modes]
        + [(NODES,) + modes] * 4
        + [(NODES,) + half] * 3,
        [modes, (NODES,) + modes, (NODES,) + modes, (NODES,) + half],
        scalar=place,
    )
    both = ("node", "space")
    count = NODES * SLABS
    held = lax.all_to_all(sent.reshape(count, 8, 128), both, 0, 0, tiled=True)
    (sent,) = run(
        middle_kernel,
        (held.reshape(16, 2, 4, 2, 8, 128), kappa, c["x_fwd"], c["x_inv"], c["y_fwd"], c["y_inv"]),
        [(16, 2, 4, 2, 8, 128)],
        [rows, (PLANES, NXY, NXY)],
    )
    held = lax.all_to_all(sent.reshape(count, 8, 128), both, 0, 0, tiled=True)
    (sent,) = run(
        functools.partial(step_kernel, shifts, quadrature),
        (held.reshape(NODES, SLABS, 8, 128), sections, start, c["z_fwd"], c["z_inv"], c["zlev0"], *weights, *tables),
        [(NODES, SLABS, 8, 128)],
        [(NODES,) + modes, (NODES,) + tile, (NODES,) + modes, (NODES,) + modes, (NODES,) + half],
        scalar=place,
    )
    held = lax.all_to_all(sent.reshape(count, 8, 128), both, 0, 0, tiled=True)
    (out,) = run(
        last_kernel,
        (held.reshape(16, 2, 4, 2, 8, 128), c["x_inv"], c["y_inv"]),
        [(1, PLANES, NXY, NXY)],
        [rows, (PLANES, NXY, NXY), pltpu.SemaphoreType.DMA((PLANES,))],
        far_out=True,
    )
    return out


def solution(mesh):
    in_specs = (P("space", None, None), P("space", None, None))
    out_specs = P("node", "space", None, None)
    return jax.shard_map(
        per_device, mesh=mesh, in_specs=in_specs, out_specs=out_specs, check_vma=False
    )
```
